32 devices in a mesh: gx: 2 (over x), gy: 4 (over z), ta: 4 (over y, core).
Axes of the slice: x: 2, y: 2, z: 4, core: 2. Of those that a mesh axis runs over, the one named last changes fastest.
Arguments:
- traces: bfloat16 [131072, 1024], P(('gx', 'gy'), 'ta'), may hold values from -6 to 6
- interp: bfloat16 [2, 16], replicated, may hold values from -1.5 to 1.5
- translations: bfloat16 [4, 2048, 1024], P(None, ('gx', 'gy')), may hold values from -0.125 to 0.125
- leaf_slot: int32 [8192], P(('gx', 'gy', 'ta')), may hold values from 0 to 255, as said below
- pairing: int32 [4, 8192], P(None, ('gx', 'gy', 'ta')), may hold values from 0 to 255, as said below
Outputs:
- coefficients: bfloat16 [8192, 1024], P(('gx', 'gy', 'ta'))
The draws below stay inside these ranges and needn't reach their ends.
Inputs may be any that keep to these rules, and one draw needn't show every extreme that they name: `leaf_slot`: each aligned block of 256 entries (the leaves of one device) is a permutation of 0 to 255. `pairing`: for every level, each aligned block of 256 entries along the leaves is a permutation of 0 to 255.
All inputs are finite; a program needn't handle non-finite values.
Results may differ from the reference program's by a relative error of at most 0.0082.
Values may be sent and summed in bfloat16 or wider, within the bound.
A program may use at most 128 MiB of HBM per device.

```python
import math
import jax
import jax.numpy as jnp
from jax import lax

NT = 1024
NF = 256
CHEB = 2
BOXT = 16
LEVELS = 4
BOX_DEV = 256
W = 1024
NBOX = 8192
NTRACE = 131072
N_GX = 2
N_GY = 4
N_TA = 4


def block_perms(key, blocks, width):
    keys = jax.random.split(key, blocks)
    return jax.vmap(lambda subkey: jax.random.permutation(subkey, width))(keys).astype(jnp.int32)


def draw_leaf_slot(key, part):
    return block_perms(jax.random.fold_in(key, 11), NBOX // BOX_DEV, BOX_DEV).reshape(NBOX)


def draw_pairing(key, part):
    return block_perms(jax.random.fold_in(key, 23), LEVELS * (NBOX // BOX_DEV), BOX_DEV).reshape(LEVELS, NBOX)


def levels(key, shape, cuts, least, largest):
    loudness = 1.0
    for dim, parts in cuts:
        draws = jax.random.uniform(jax.random.fold_in(jax.random.fold_in(key, 6), dim), (parts,), jnp.float32, least / len(cuts), largest / len(cuts))
        loudness = loudness * jnp.repeat(jnp.exp(draws), shape[dim] // parts).reshape((-1,) + (1,) * (len(shape) - 1 - dim))
    return loudness


def scatter_about(key, extent, scale, limit, pieces=(), kind=jnp.bfloat16):
    level = levels(key, extent, pieces, -0.22, 0.18) if pieces else 1.0
    values = jax.random.normal(key, extent, jnp.float32) * scale * level
    return jnp.minimum(jnp.maximum(values, -limit), limit).astype(kind)


def setup_inputs(seed: int = 0) -> dict:
    splits = jax.random.split(jax.random.key(seed), 6)
    return {
        "traces": scatter_about(splits[0], (NTRACE, NT), 1.0, 6.0, ((0, 8), (1, 4))),
        "interp": scatter_about(splits[1], (CHEB, BOXT), BOXT ** -0.5, 1.5),
        "translations": scatter_about(splits[2], (LEVELS, 2 * W, W), (2 * W) ** -0.5, 0.125, ((1, 8),)),
        "leaf_slot": draw_leaf_slot(jax.random.fold_in(splits[5], 71), 0),
        "pairing": draw_pairing(jax.random.fold_in(splits[5], 71), 0),
    }


def spectrum_table(length, count):
    sample_pos = lax.broadcasted_iota(jnp.float32, (length, count), 0)
    frequency = lax.broadcasted_iota(jnp.float32, (length, count), 1) + 1.0
    angles = 2.0 * math.pi / length * jnp.mod(sample_pos * frequency, float(length))
    factor = math.sqrt(2.0 / length)
    return jnp.concatenate([jnp.cos(angles) * factor, -jnp.sin(angles) * factor], axis=1).astype(jnp.bfloat16)

def reference(traces, interp, translations, leaf_slot, pairing):
    devices = N_GX * N_GY * N_TA
    groups = N_GX * N_GY
    per_peer = BOX_DEV // groups
    fourier = spectrum_table(NT, NF)
    weights = interp.astype(jnp.float32)

    def one_device(device_block):
        sampled = jnp.einsum('cb,kbt->kct', weights, device_block.astype(jnp.float32), precision=lax.Precision.HIGHEST)
        sampled = sampled.astype(jnp.bfloat16).reshape(BOX_DEV * CHEB, NT)
        spectra = jnp.dot(sampled, fourier, preferred_element_type=jnp.float32)
        return spectra.reshape(BOX_DEV, CHEB * 2 * NF).astype(jnp.bfloat16)
    cheb_points = lax.map(one_device, traces.reshape(devices, BOX_DEV, BOXT, NT))
    cheb_points = cheb_points.reshape(NBOX, CHEB * 2 * NF)
    leaves = jnp.arange(NBOX, dtype=jnp.int32)
    owners = leaves // BOX_DEV
    group_index = owners // N_TA
    ta_index = owners % N_TA
    source_group = leaf_slot // per_peer
    offset = leaf_slot % per_peer
    source_rows = ((source_group * N_TA + ta_index) * BOX_DEV + group_index * per_peer + offset).astype(jnp.int32)
    states = cheb_points[source_rows]
    log_devices = devices.bit_length() - 1
    for layer_index in range(LEVELS):
        flip_bit = layer_index * log_devices // LEVELS
        partner = ((owners ^ 1 << flip_bit) * BOX_DEV + pairing[layer_index]).astype(jnp.int32)
        joined = jnp.concatenate([states, states[partner]], axis=1).astype(jnp.float32)
        product_sum = jnp.dot(joined, translations[layer_index].astype(jnp.float32), precision=lax.Precision.HIGHEST)
        states = product_sum.astype(jnp.bfloat16)
    return states
```

```python
import functools
import math

import jax
import jax.numpy as jnp
import numpy as np
from jax import lax
from jax.experimental import pallas as pl
from jax.experimental.pallas import tpu as pltpu
from jax.sharding import PartitionSpec as P

NF = 256
CHEB = 2
BOXT = 16
BLOCK_BOXES = 16
TILE = 256
MESH = pl.DeviceIdType.MESH
KEPT = (0.625, 0.625, 0.75, 0.75)
SCHEDULE = {
    "start": ((0, 0), (1, 0)),
    "interp0": ((0, 1),),
    "table2": ((1, 1),),
    "spread": ((0, 2), (2, 0), (1, 1), (0, 3), (1, 2), (0, 4), (2, 1)),
    "level0.0": ((1, 3), (3, 0)),
    "level1.0": ((2, 2), (3, 1)),
    "level1.1": ((2, 3),),
    "level1.2": ((3, 2),),
    "level2.0": ((3, 3),),
}


def spectrum_table(length, count):
    sample_pos = np.arange(length, dtype=np.float32)[:, None]
    frequency = np.arange(count, dtype=np.float32)[None, :] + np.float32(1.0)
    angles = np.float32(2.0 * math.pi / length) * np.mod(sample_pos * frequency, np.float32(length))
    factor = np.float32(math.sqrt(2.0 / length))
    table = np.concatenate([np.cos(angles) * factor, -np.sin(angles) * factor], axis=1)
    return table.astype(jnp.bfloat16)


def flip(index, mask, size):
    result = index
    bit = 1
    while bit < size:
        if mask & bit:
            result = result + bit - 2 * bit * ((index // bit) % 2)
        bit *= 2
    return result


def kernel(
    sizes,
    traces,
    interp,
    translations,
    slots,
    pairs,
    table,
    out,
    tr,
    weights,
    mat,
    sampled,
    slices,
    fourier,
    acc,
    points,
    arrived,
    states,
    partner,
    select,
    load_sem,
    table_sem,
    own_sem,
    ag_send,
    ag_recv,
    z_send,
    x_send,
    y_send,
    y_recv,
    core_send,
    core_recv,
    ta_send,
    ta_recv,
    g_send,
    g_recv,
    level_send,
    level_recv,
):
    n_gx, n_gy, n_ta = sizes
    groups = n_gx * n_gy
    gx, gy, ta = lax.axis_index("gx"), lax.axis_index("gy"), lax.axis_index("ta")
    group = gx * n_gy + gy
    level_count = translations.shape[0]
    rows = translations.shape[1]
    half = rows // 2
    width = translations.shape[2]
    boxes = slots.shape[1]
    span = traces.shape[1]
    block = boxes * BOXT
    chunk = states.shape[3]
    chunks = width // chunk
    log_devices = (groups * n_ta).bit_length() - 1
    side = ta % 2

    def of_group(offset):
        p = flip(group, offset, groups)
        return (p // n_gy, p % n_gy, ta)

    def of_ta(offset):
        return (gx, gy, flip(ta, offset, n_ta))

    def loading(j):
        t = flip(ta, j, n_ta)
        return pltpu.make_async_copy(
            traces.at[pl.ds(pl.multiple_of(t * block, block), block), :], tr.at[j], load_sem.at[j]
        )

    def own(level):
        return [
            pltpu.make_async_copy(
                translations.at[level, pl.ds(part * half, half), :],
                weights.at[level, group, part],
                own_sem.at[level, part],
            )
            for part in range(2)
        ]

    xbits = []
    bit = n_gx // 2
    while bit:
        xbits.append(bit)
        bit //= 2
    stage_of = {0: -1}
    for stage, bit in enumerate(xbits):
        for offset in list(stage_of):
            stage_of[offset ^ bit] = stage
    lines = {offset: flip(gx, offset, n_gx) for offset in stage_of}
    shards = [
        (offset, d, k)
        for k in range(-1, n_gy - 1)
        for d in ((1,) if k < 0 else (1, -1))
        for offset in stage_of
    ]
    twins = n_ta >= 4
    twin = flip(ta, 2, n_ta) if twins else ta
    upper = (ta // 2) % 2

    def kept(level):
        if not twins:
            return half
        return max(half // 2, round(half * KEPT[level % len(KEPT)] / 16) * 16)

    def shard_id(offset, d, k):
        return lines[offset] * n_gy + gy - d * (k + 1)

    within = {
        (d, k): gy >= k + 1 if d > 0 else gy < n_gy - 1 - k
        for d in (1, -1)
        for k in range(n_gy - 1)
    }
    ahead = {1: gy < n_gy - 1, -1: gy > 0}

    def inside(d, k):
        return None if k < 0 else within[d, k]

    def both(a, b):
        if a is None or b is None:
            return b if a is None else a
        return jnp.logical_and(a, b)

    def guarded(condition, action):
        if condition is None:
            action()
        else:
            pl.when(condition)(action)

    started = []

    def launch(condition, make, outer=None):
        guarded(condition, lambda: make().start())
        started.append((outer, condition, make))

    def in_rows(level):
        size = kept(level)
        if size == half:
            return pl.ds(0, half)
        return pl.ds(pl.multiple_of(upper * (half - size), 16), size)

    def in_plane(level, shard, sem_ref, sem_at, target):
        place = weights.at[level, shard, side, in_rows(level), :]
        return pltpu.make_async_remote_copy(
            src_ref=place,
            dst_ref=place,
            send_sem=sem_ref.at[sem_at],
            recv_sem=ag_recv.at[level, shard],
            device_id=target,
            device_id_type=MESH,
        )

    def z_copy(level, shard, d):
        return in_plane(level, shard, z_send, (level, (d + 1) // 2, shard), (gx, gy + d, ta))

    def x_copy(level, shard, stage):
        target = (lines[xbits[stage]], gy, ta)
        return in_plane(level, shard, x_send, (level, stage, shard), target)

    def y_copy(level, shard, sending):
        size = kept(level)
        first = (upper if sending else 1 - upper) * size
        place = weights.at[level, shard, side, pl.ds(pl.multiple_of(first, 16), half - size), :]
        return pltpu.make_async_remote_copy(
            src_ref=place,
            dst_ref=place,
            send_sem=y_send.at[level, shard],
            recv_sem=y_recv.at[level, shard],
            device_id=(gx, gy, twin),
            device_id_type=MESH,
        )

    def core_copy(level, shard, kind, mine):
        size = kept(level)
        if kind == 0:
            rows_at = in_rows(level)
        else:
            rows_at = pl.ds(pl.multiple_of((1 - upper) * size, 16), half - size)
        place = weights.at[level, shard, side if mine else 1 - side, rows_at, :]
        return pltpu.make_async_remote_copy(
            src_ref=place,
            dst_ref=place,
            send_sem=core_send.at[level, kind, shard],
            recv_sem=core_recv.at[level, kind, shard],
            device_id=of_ta(1),
            device_id_type=MESH,
        )

    def hops(offset, k):
        return k + 1 + bin(offset).count("1")

    def has_twin(level):
        return kept(level) < half

    def forward(level, offset, d, k):
        shard = shard_id(offset, d, k)
        valid = inside(d, k)
        own_shard = offset == 0 and k < 0

        def body():
            if not own_shard:
                in_plane(level, shard, ag_send, 0, of_ta(1)).wait_recv()
                launch(None, lambda: core_copy(level, shard, 0, True), valid)
            if offset == 0:
                for way in (1, -1) if k < 0 else (d,):
                    launch(ahead[way], lambda way=way: z_copy(level, shard, way), valid)
            for stage in range(stage_of[offset] + 1, len(xbits)):
                launch(None, lambda stage=stage: x_copy(level, shard, stage), valid)
            if has_twin(level) and not own_shard:
                launch(None, lambda: y_copy(level, shard, True), valid)

        guarded(valid, body)

    def crossed(level, offset, d, k):
        shard = shard_id(offset, d, k)

        def body():
            y_copy(level, shard, False).wait_recv()
            launch(None, lambda: core_copy(level, shard, 1, True), inside(d, k))

        guarded(inside(d, k), body)

    last_round = n_gy - 1 + len(xbits) + 1

    def pump(level, step):
        if step == 0:
            for copy in own(level):
                copy.wait()
        for offset, d, k in shards:
            if has_twin(level) and hops(offset, k) == step - 1 and (offset or k >= 0):
                crossed(level, offset, d, k)
            if hops(offset, k) == step:
                forward(level, offset, d, k)

    pumped = {}

    def pumps(point):
        for level, upto in SCHEDULE.get(point, ()):
            if level < level_count:
                pump_to(level, min(upto, last_round))

    def pump_to(level, upto):
        while pumped.get(level, -1) < upto:
            pumped[level] = pumped.get(level, -1) + 1
            pump(level, pumped[level])

    def finish(level):
        pump_to(level, last_round)
        for offset, d, k in shards:
            if offset == 0 and k < 0:
                continue

            def body():
                core_copy(level, shard_id(offset, d, k), 0, False).wait_recv()
                if has_twin(level):
                    core_copy(level, shard_id(offset, d, k), 1, False).wait_recv()

            guarded(inside(d, k), body)

    def regroup(j):
        return pltpu.make_async_remote_copy(
            src_ref=sampled.at[j],
            dst_ref=slices.at[j],
            send_sem=ta_send.at[j],
            recv_sem=ta_recv.at[j],
            device_id=of_ta(j),
            device_id_type=MESH,
        )

    def moving(offset, sending):
        src = points.at[flip(group, offset, groups)]
        dst = arrived.at[group if sending else flip(group, offset, groups)]
        return pltpu.make_async_remote_copy(
            src_ref=src,
            dst_ref=dst,
            send_sem=g_send.at[offset],
            recv_sem=g_recv.at[offset],
            device_id=of_group(offset),
            device_id_type=MESH,
        )

    def exchange(level, k):
        mask = 2 ** (level * log_devices // level_count)
        target = of_ta(mask) if mask < n_ta else of_group(mask // n_ta)
        return pltpu.make_async_remote_copy(
            src_ref=states.at[level, k],
            dst_ref=partner.at[level, k],
            send_sem=level_send.at[level, k],
            recv_sem=level_recv.at[level, k],
            device_id=target,
            device_id_type=MESH,
        )

    near = [n_ta - 1 - j for j in range(n_ta)]
    for j in near:
        loading(j).start()
    for level in range(level_count):
        for copy in own(level):
            copy.start()
    table_copy = pltpu.make_async_copy(table, fourier, table_sem)
    table_copy.start()

    barrier = pltpu.get_barrier_semaphore()
    for j in range(1, n_ta):
        pl.semaphore_signal(barrier, inc=1, device_id=of_ta(j), device_id_type=MESH)
    for offset in range(1, groups):
        pl.semaphore_signal(barrier, inc=1, device_id=of_group(offset), device_id_type=MESH)

    columns = BLOCK_BOXES * BOXT
    spread = (
        lax.broadcasted_iota(jnp.int32, (BOXT, columns), 1) % BOXT
        == lax.broadcasted_iota(jnp.int32, (BOXT, columns), 0)
    )
    tiled = jnp.dot(
        interp[...], spread.astype(jnp.float32).astype(jnp.bfloat16), preferred_element_type=jnp.float32
    )
    own_box = (
        lax.broadcasted_iota(jnp.int32, (BLOCK_BOXES, columns), 1) // BOXT
        == lax.broadcasted_iota(jnp.int32, (BLOCK_BOXES, columns), 0)
    )
    for c in range(CHEB):
        mat[pl.ds(c * BLOCK_BOXES, BLOCK_BOXES), :] = jnp.where(
            own_box, tiled[c : c + 1, :], 0.0
        ).astype(jnp.bfloat16)

    def selection(index_row):
        hit = lax.broadcasted_iota(jnp.int32, (boxes, boxes), 0) == index_row
        return jnp.where(hit, 1.0, 0.0).T.astype(jnp.bfloat16)

    select[0] = selection(slots[...])
    for level in range(level_count):
        select[level + 1] = selection(pairs[pl.ds(level, 1), :])

    pl.semaphore_wait(barrier, n_ta - 1 + groups - 1)
    pumps("start")

    for j in near:
        loading(j).wait()
        where = sampled if j else slices

        def interpolate(i, carry):
            traces_block = tr[j, pl.ds(pl.multiple_of(i * columns, columns), columns), :]
            both = jnp.dot(mat[...], traces_block, preferred_element_type=jnp.float32)
            both = both.astype(jnp.bfloat16)
            place = pl.ds(pl.multiple_of(i * BLOCK_BOXES, BLOCK_BOXES), BLOCK_BOXES)
            for c in range(CHEB):
                where[j, c, place, :] = both[c * BLOCK_BOXES : (c + 1) * BLOCK_BOXES, :]
            return carry

        lax.fori_loop(0, boxes // BLOCK_BOXES, interpolate, 0, unroll=4)
        if j:
            regroup(j).start()
        pumps(f"interp{j}")

    table_copy.wait()
    for j in range(n_ta):
        if j:
            pumps(f"table{j}")
            regroup(j).wait_recv()
        first = pl.multiple_of(flip(ta, j, n_ta) * span, span)
        for c in range(CHEB):
            part = jnp.dot(
                slices[j, c], fourier[pl.ds(first, span), :], preferred_element_type=jnp.float32
            )
            cols = pl.ds(c * 2 * NF, 2 * NF)
            if j:
                acc[:, cols] += part
            else:
                acc[:, cols] = part
    points[...] = acc[...].reshape(points.shape).astype(jnp.bfloat16)
    for offset in range(groups - 1, 0, -1):
        moving(offset, True).start()
    arrived[group] = points[group]
    pumps("spread")
    for offset in range(1, groups):
        moving(offset, False).wait_recv()

    for k in range(chunks):
        boxes_in = arrived[:, :, k * chunk : (k + 1) * chunk].astype(jnp.float32)
        boxes_in = boxes_in.reshape(boxes, chunk).astype(jnp.bfloat16)
        states[0, k] = jnp.dot(select[0], boxes_in, preferred_element_type=jnp.float32).astype(
            jnp.bfloat16
        )
        exchange(0, k).start()

    per_chunk = chunk // rows

    def weight(level, k, cols):
        piece = weights[level, k * per_chunk : (k + 1) * per_chunk, :, :, cols]
        return piece.reshape(chunk, chunk)

    for level in range(level_count):
        finish(level)

        def own_part(n, carry):
            cols = pl.ds(pl.multiple_of(n * chunk, chunk), chunk)
            total = jnp.zeros((boxes, chunk), jnp.float32)
            for k in range(chunks):
                total += jnp.dot(
                    states[level, k], weight(level, k, cols), preferred_element_type=jnp.float32
                )
            acc[:, cols] = total
            return carry

        lax.fori_loop(0, chunks, own_part, 0)
        for k in range(chunks):
            pumps(f"level{level}.{k}")
            exchange(level, k).wait_recv()
            aligned = jnp.dot(
                select[level + 1], partner[level, k], preferred_element_type=jnp.float32
            ).astype(jnp.bfloat16)
            if k < chunks - 1:

                def partner_part(n, carry):
                    cols = pl.ds(pl.multiple_of(n * chunk, chunk), chunk)
                    acc[:, cols] += jnp.dot(
                        aligned, weight(level, chunks + k, cols), preferred_element_type=jnp.float32
                    )
                    return carry

                lax.fori_loop(0, chunks, partner_part, 0)
            else:
                for n in range(chunks):
                    cols = pl.ds(n * chunk, chunk)
                    total = acc[:, cols] + jnp.dot(
                        aligned, weight(level, chunks + k, cols), preferred_element_type=jnp.float32
                    )
                    if level < level_count - 1:
                        states[level + 1, n] = total.astype(jnp.bfloat16)
                        exchange(level + 1, n).start()
                    else:
                        out[:, cols] = total.astype(jnp.bfloat16)

    for j in range(1, n_ta):
        regroup(j).wait_send()
    for offset in range(1, groups):
        moving(offset, True).wait_send()
    for level in range(level_count):
        for k in range(chunks):
            exchange(level, k).wait_send()
    for outer, condition, make in started:
        guarded(both(outer, condition), lambda: make().wait_send())


def on_device(sizes, traces, interp, translations, leaf_slot, pairing):
    n_gx, n_gy, n_ta = sizes
    groups = n_gx * n_gy
    boxes = leaf_slot.shape[0]
    levels, rows, width = translations.shape
    span = traces.shape[1]
    block = traces.shape[0] // n_ta
    chunk = max(TILE, rows)
    chunks = width // chunk
    table = jnp.asarray(spectrum_table(span * n_ta, NF))
    bf16, f32 = jnp.bfloat16, jnp.float32
    anywhere = pl.BlockSpec(memory_space=pl.ANY)
    vmem = pl.BlockSpec(memory_space=pltpu.VMEM)
    dma = pltpu.SemaphoreType.DMA
    return pl.pallas_call(
        functools.partial(kernel, sizes),
        out_shape=jax.ShapeDtypeStruct((boxes, width), bf16),
        in_specs=[anywhere, vmem, anywhere, vmem, vmem, anywhere],
        out_specs=vmem,
        scratch_shapes=[
            pltpu.VMEM((n_ta, block, span), bf16),
            pltpu.VMEM((levels, groups, 2, rows // 2, width), bf16),
            pltpu.VMEM((CHEB * BLOCK_BOXES, BLOCK_BOXES * BOXT), bf16),
            pltpu.VMEM((n_ta, CHEB, boxes, span), bf16),
            pltpu.VMEM((n_ta, CHEB, boxes, span), bf16),
            pltpu.VMEM(table.shape, bf16),
            pltpu.VMEM((boxes, width), f32),
            pltpu.VMEM((groups, boxes // groups, width), bf16),
            pltpu.VMEM((groups, boxes // groups, width), bf16),
            pltpu.VMEM((levels, chunks, boxes, chunk), bf16),
            pltpu.VMEM((levels, chunks, boxes, chunk), bf16),
            pltpu.VMEM((levels + 1, boxes, boxes), bf16),
            dma((n_ta,)),
            dma,
            dma((levels, 2)),
            dma((1,)),
            dma((levels, groups)),
            dma((levels, 2, groups)),
            dma((levels, max(1, n_gx.bit_length() - 1), groups)),
            dma((levels, groups)),
            dma((levels, groups)),
            dma((levels, 2, groups)),
            dma((levels, 2, groups)),
            dma((n_ta,)),
            dma((n_ta,)),
            dma((groups,)),
            dma((groups,)),
            dma((levels, chunks)),
            dma((levels, chunks)),
        ],
        compiler_params=pltpu.CompilerParams(
            collective_id=0, has_side_effects=True, vmem_limit_bytes=60 * 2**20
        ),
    )(traces, interp, translations, leaf_slot.reshape(1, boxes), pairing, table)


def solution(mesh):
    sizes = (mesh.shape["gx"], mesh.shape["gy"], mesh.shape["ta"])
    in_specs = (
        P(("gx", "gy"), "ta"),
        P(),
        P(None, ("gx", "gy"), None),
        P(("gx", "gy", "ta")),
        P(None, ("gx", "gy", "ta")),
    )
    out_specs = P(("gx", "gy", "ta"), None)
    return jax.shard_map(
        functools.partial(on_device, sizes),
        mesh=mesh,
        in_specs=in_specs,
        out_specs=out_specs,
        check_vma=False,
    )
```

```python
import functools
import math

import jax
import jax.numpy as jnp
import numpy as np
from jax import lax
from jax.experimental import pallas as pl
from jax.experimental.pallas import tpu as pltpu
from jax.sharding import PartitionSpec as P

NF = 256
CHEB = 2
BOXT = 16
BLOCK_BOXES = 16
TILE = 256
MESH = pl.DeviceIdType.MESH
KEPT = (0.5, 0.75, 1, 0.5)
SCHEDULE = {
    "start": ((0, 0, 0, -1),),
    "interp1": ((0, 1, 0, -1), (0, 0, 0, 0), (0, 1, 0, 0),),
    "interp3": ((0, 0, 0, 1), (1, 0, 0, 0), (1, 1, 0, 0), (0, 1, 0, 1), (0, 0, 0, 2),),
    "table2": ((0, 0, 1, 0), (0, 0, 1, 2),),
    "spread2": (
        (0, 0, 1, 1),
        (1, 2, 1, 2),
        (0, 1, 0, 2),
        (1, 0, 0, 2),
        (1, 2, 0, 2),
        (1, 2, 1, 0),
    ),
    "table3": ((1, 0, 1, 0),),
    "spread3": (
        (0, 2, 0, -1),
        (0, 0, 1, -1),
        (0, 1, 1, -1),
        (1, 0, 1, 1),
        (1, 2, 0, 1),
        (0, 1, 1, 0),
        (0, 1, 1, 1),
    ),
    "spread": ((1, 0, 0, 1), (1, 1, 0, 1), (0, 3, 0, -1), (0, 1, 1, 2), (1, 0, 1, 2),),
    "own0": ((1, 0, 1, -1),),
    "level0.1": ((0, 2, 0, 0),),
    "own1": (
        (1, 1, 1, 0),
        (0, 2, 1, -1),
        (0, 2, 0, 1),
        (1, 1, 1, -1),
        (1, 1, 0, 2),
        (1, 1, 1, 2),
        (1, 1, 1, 1),
    ),
    "level1.0": ((1, 2, 1, -1),),
    "level1.2": ((0, 2, 0, 2), (0, 3, 0, 0),),
    "level1.3": ((0, 2, 1, 0),),
    "own2": ((0, 2, 1, 1), (0, 3, 0, 1), (1, 2, 0, 0), (1, 2, 1, 1), (0, 2, 1, 2),),
    "level2.0": ((0, 3, 1, -1),),
    "level2.1": ((1, 3, 0, 1),),
    "level2.3": ((0, 3, 1, 1), (1, 3, 0, 0),),
    "own3": (
        (0, 3, 1, 0),
        (1, 3, 1, -1),
        (0, 3, 0, 2),
        (1, 3, 0, 2),
        (0, 3, 1, 2),
        (1, 3, 1, 2),
        (1, 3, 1, 1),
        (1, 3, 1, 0),
    ),
}


def spectrum_table(length, count):
    sample_pos = np.arange(length, dtype=np.float32)[:, None]
    frequency = np.arange(count, dtype=np.float32)[None, :] + np.float32(1.0)
    angles = np.float32(2.0 * math.pi / length) * np.mod(sample_pos * frequency, np.float32(length))
    factor = np.float32(math.sqrt(2.0 / length))
    table = np.concatenate([np.cos(angles) * factor, -np.sin(angles) * factor], axis=1)
    return table.astype(jnp.bfloat16)


def flip(index, mask, size):
    result = index
    bit = 1
    while bit < size:
        if mask & bit:
            result = result + bit - 2 * bit * ((index // bit) % 2)
        bit *= 2
    return result


def kernel(
    sizes,
    traces,
    interp,
    translations,
    slots,
    pairs,
    table,
    out,
    tr,
    weights,
    mat,
    sampled,
    slices,
    fourier,
    acc,
    points,
    arrived,
    states,
    partner,
    select,
    load_sem,
    table_sem,
    own_sem,
    ag_send,
    ag_recv,
    z_send,
    x_send,
    y_send,
    y_recv,
    core_send,
    core_recv,
    ta_send,
    ta_recv,
    g_send,
    g_recv,
    level_send,
    level_recv,
):
    n_gx, n_gy, n_ta = sizes
    groups = n_gx * n_gy
    gx, gy, ta = lax.axis_index("gx"), lax.axis_index("gy"), lax.axis_index("ta")
    group = gx * n_gy + gy
    level_count = translations.shape[0]
    rows = translations.shape[1]
    half = rows // 2
    width = translations.shape[2]
    boxes = slots.shape[1]
    span = traces.shape[1]
    block = boxes * BOXT
    chunk = states.shape[3]
    chunks = width // chunk
    log_devices = (groups * n_ta).bit_length() - 1
    side = ta % 2

    def of_group(offset):
        p = flip(group, offset, groups)
        return (p // n_gy, p % n_gy, ta)

    def of_ta(offset):
        return (gx, gy, flip(ta, offset, n_ta))

    def loading(j):
        t = flip(ta, j, n_ta)
        return pltpu.make_async_copy(
            traces.at[pl.ds(pl.multiple_of(t * block, block), block), :], tr.at[j], load_sem.at[j]
        )

    def own(level):
        return [
            pltpu.make_async_copy(
                translations.at[level, pl.ds(part * half, half), :],
                weights.at[level, group, part],
                own_sem.at[level, part],
            )
            for part in range(2)
        ]

    xbits = []
    bit = n_gx // 2
    while bit:
        xbits.append(bit)
        bit //= 2
    stage_of = {0: -1}
    for stage, bit in enumerate(xbits):
        for offset in list(stage_of):
            stage_of[offset ^ bit] = stage
    lines = {offset: flip(gx, offset, n_gx) for offset in stage_of}
    shards = [
        (offset, d, k)
        for k in range(-1, n_gy - 1)
        for d in ((1,) if k < 0 else (1, -1))
        for offset in stage_of
    ]
    twins = n_ta >= 4
    twin = flip(ta, 2, n_ta) if twins else ta
    upper = (ta // 2) % 2

    def kept(level):
        if not twins:
            return half
        return max(half // 2, round(half * KEPT[level % len(KEPT)] / 16) * 16)

    def shard_id(offset, d, k):
        return lines[offset] * n_gy + gy - d * (k + 1)

    within = {
        (d, k): gy >= k + 1 if d > 0 else gy < n_gy - 1 - k
        for d in (1, -1)
        for k in range(n_gy - 1)
    }
    ahead = {1: gy < n_gy - 1, -1: gy > 0}

    def inside(d, k):
        return None if k < 0 else within[d, k]

    def both(a, b):
        if a is None or b is None:
            return b if a is None else a
        return jnp.logical_and(a, b)

    def guarded(condition, action):
        if condition is None:
            action()
        else:
            pl.when(condition)(action)

    started = []

    def launch(condition, make, outer=None):
        guarded(condition, lambda: make().start())
        started.append((outer, condition, make))

    def in_rows(level):
        size = kept(level)
        if size == half:
            return pl.ds(0, half)
        return pl.ds(pl.multiple_of(upper * (half - size), 16), size)

    def in_plane(level, shard, sem_ref, sem_at, target):
        place = weights.at[level, shard, side, in_rows(level), :]
        return pltpu.make_async_remote_copy(
            src_ref=place,
            dst_ref=place,
            send_sem=sem_ref.at[sem_at],
            recv_sem=ag_recv.at[level, shard],
            device_id=target,
            device_id_type=MESH,
        )

    def z_copy(level, shard, d):
        return in_plane(level, shard, z_send, (level, (d + 1) // 2, shard), (gx, gy + d, ta))

    def x_copy(level, shard, stage):
        target = (lines[xbits[stage]], gy, ta)
        return in_plane(level, shard, x_send, (level, stage, shard), target)

    def y_copy(level, shard, sending):
        size = kept(level)
        first = (upper if sending else 1 - upper) * size
        place = weights.at[level, shard, side, pl.ds(pl.multiple_of(first, 16), half - size), :]
        return pltpu.make_async_remote_copy(
            src_ref=place,
            dst_ref=place,
            send_sem=y_send.at[level, shard],
            recv_sem=y_recv.at[level, shard],
            device_id=(gx, gy, twin),
            device_id_type=MESH,
        )

    def core_copy(level, shard, kind, mine):
        size = kept(level)
        if kind == 0:
            rows_at = in_rows(level)
        else:
            rows_at = pl.ds(pl.multiple_of((1 - upper) * size, 16), half - size)
        place = weights.at[level, shard, side if mine else 1 - side, rows_at, :]
        return pltpu.make_async_remote_copy(
            src_ref=place,
            dst_ref=place,
            send_sem=core_send.at[level, kind, shard],
            recv_sem=core_recv.at[level, kind, shard],
            device_id=of_ta(1),
            device_id_type=MESH,
        )

    def has_twin(level):
        return kept(level) < half

    def forward(level, offset, d, k):
        shard = shard_id(offset, d, k)
        valid = inside(d, k)
        own_shard = offset == 0 and k < 0

        def body():
            if not own_shard:
                in_plane(level, shard, ag_send, 0, of_ta(1)).wait_recv()
                launch(None, lambda: core_copy(level, shard, 0, True), valid)
            if offset == 0:
                for way in (1, -1) if k < 0 else (d,):
                    launch(ahead[way], lambda way=way: z_copy(level, shard, way), valid)
            for stage in range(stage_of[offset] + 1, len(xbits)):
                launch(None, lambda stage=stage: x_copy(level, shard, stage), valid)
            if has_twin(level) and not own_shard:
                launch(None, lambda: y_copy(level, shard, True), valid)

        guarded(valid, body)

    def crossed(level, offset, d, k):
        shard = shard_id(offset, d, k)

        def body():
            y_copy(level, shard, False).wait_recv()
            launch(None, lambda: core_copy(level, shard, 1, True), inside(d, k))

        guarded(inside(d, k), body)

    handled = set()

    def piece(across, level, over, k):
        if (across, level, over, k) in handled or level >= level_count or k > n_gy - 2:
            return
        handled.add((across, level, over, k))
        if not (across or over) and k >= 0:
            piece(0, level, 0, k - 1)
        if across and not has_twin(level):
            return
        if k < 0 and not (across or over):
            for copy in own(level):
                copy.wait()
        for offset, d, at in shards:
            if at == k and (offset > 0) == (over > 0):
                if not across:
                    forward(level, offset, d, k)
                elif offset or k >= 0:
                    crossed(level, offset, d, k)

    def pumps(point):
        for entry in SCHEDULE.get(point, ()):
            piece(*entry)

    def flush(level):
        for across in range(2):
            for total in range(-1, n_gy):
                for over in range(2):
                    if -1 <= total - over < n_gy - 1:
                        piece(across, level, over, total - over)

    def finish(level, first, count):
        for shard in range(first, first + count):

            def body():
                core_copy(level, shard, 0, False).wait_recv()
                if has_twin(level):
                    core_copy(level, shard, 1, False).wait_recv()

            pl.when(group != shard)(body)

    portions = min(4, groups)
    per_portion = groups // portions
    portion_rows = boxes // portions
    portion_order = sorted(range(portions), key=lambda c: (-(c % 2), -c))

    def portion(c):
        return flip(group // per_portion, c, portions)

    def portion_at(c):
        return pl.multiple_of(portion(c) * portion_rows, portion_rows)

    def regroup(j, c):
        place = pl.ds(portion_at(c), portion_rows)
        return pltpu.make_async_remote_copy(
            src_ref=sampled.at[j, :, place, :],
            dst_ref=slices.at[j, :, place, :],
            send_sem=ta_send.at[j, c],
            recv_sem=ta_recv.at[j, c],
            device_id=of_ta(j),
            device_id_type=MESH,
        )

    def moving(offset, sending):
        src = points.at[flip(group, offset, groups)]
        dst = arrived.at[group if sending else flip(group, offset, groups)]
        return pltpu.make_async_remote_copy(
            src_ref=src,
            dst_ref=dst,
            send_sem=g_send.at[offset],
            recv_sem=g_recv.at[offset],
            device_id=of_group(offset),
            device_id_type=MESH,
        )

    def exchange(level, k):
        mask = 2 ** (level * log_devices // level_count)
        target = of_ta(mask) if mask < n_ta else of_group(mask // n_ta)
        return pltpu.make_async_remote_copy(
            src_ref=states.at[level, k],
            dst_ref=partner.at[level, k],
            send_sem=level_send.at[level, k],
            recv_sem=level_recv.at[level, k],
            device_id=target,
            device_id_type=MESH,
        )

    near = [n_ta - 1 - j for j in range(n_ta)]
    for j in near:
        loading(j).start()
    for level in range(level_count):
        for copy in own(level):
            copy.start()
    table_copy = pltpu.make_async_copy(table, fourier, table_sem)
    table_copy.start()

    barrier = pltpu.get_barrier_semaphore()
    for j in range(1, n_ta):
        pl.semaphore_signal(barrier, inc=1, device_id=of_ta(j), device_id_type=MESH)
    for offset in range(1, groups):
        pl.semaphore_signal(barrier, inc=1, device_id=of_group(offset), device_id_type=MESH)

    columns = BLOCK_BOXES * BOXT
    spread = (
        lax.broadcasted_iota(jnp.int32, (BOXT, columns), 1) % BOXT
        == lax.broadcasted_iota(jnp.int32, (BOXT, columns), 0)
    )
    tiled = jnp.dot(
        interp[...], spread.astype(jnp.float32).astype(jnp.bfloat16), preferred_element_type=jnp.float32
    )
    own_box = (
        lax.broadcasted_iota(jnp.int32, (BLOCK_BOXES, columns), 1) // BOXT
        == lax.broadcasted_iota(jnp.int32, (BLOCK_BOXES, columns), 0)
    )
    for c in range(CHEB):
        mat[pl.ds(c * BLOCK_BOXES, BLOCK_BOXES), :] = jnp.where(
            own_box, tiled[c : c + 1, :], 0.0
        ).astype(jnp.bfloat16)

    def selection(index_row):
        hit = lax.broadcasted_iota(jnp.int32, (boxes, boxes), 0) == index_row
        return jnp.where(hit, 1.0, 0.0).T.astype(jnp.bfloat16)

    select[0] = selection(slots[...])
    for level in range(level_count):
        select[level + 1] = selection(pairs[pl.ds(level, 1), :])

    pl.semaphore_wait(barrier, n_ta - 1 + groups - 1)
    pumps("start")

    for turn, c in enumerate(portion_order):
        for j in near:
            if turn == 0:
                loading(j).wait()
            where = sampled if j else slices
            for i in range(portion_rows // BLOCK_BOXES):
                box = pl.multiple_of(portion_at(c) + i * BLOCK_BOXES, BLOCK_BOXES)
                traces_block = tr[j, pl.ds(pl.multiple_of(box * BOXT, columns), columns), :]
                pair = jnp.dot(mat[...], traces_block, preferred_element_type=jnp.float32)
                pair = pair.astype(jnp.bfloat16)
                for q in range(CHEB):
                    where[j, q, pl.ds(box, BLOCK_BOXES), :] = pair[
                        q * BLOCK_BOXES : (q + 1) * BLOCK_BOXES, :
                    ]
            if j:
                regroup(j, c).start()
        pumps(f"interp{turn}")

    table_copy.wait()
    for turn, c in enumerate(portion_order):
        pumps(f"table{turn}")
        place = pl.ds(portion_at(c), portion_rows)
        total = jnp.zeros((CHEB * portion_rows, 2 * NF), jnp.float32)
        for j in range(n_ta):
            if j:
                regroup(j, c).wait_recv()
            first = pl.multiple_of(flip(ta, j, n_ta) * span, span)
            part = slices[j, :, place, :].reshape(CHEB * portion_rows, span)
            total += jnp.dot(part, fourier[pl.ds(first, span), :], preferred_element_type=jnp.float32)
        mine = pl.ds(portion(c) * per_portion, per_portion)
        for q in range(CHEB):
            points[mine, :, q * 2 * NF : (q + 1) * 2 * NF] = (
                total[q * portion_rows : (q + 1) * portion_rows, :]
                .reshape(per_portion, boxes // groups, 2 * NF)
                .astype(jnp.bfloat16)
            )
        for offset in range((c + 1) * per_portion - 1, c * per_portion - 1, -1):
            if offset:
                moving(offset, True).start()
        pumps(f"spread{turn}")
    arrived[group] = points[group]
    pumps("spread")
    for offset in range(1, groups):
        moving(offset, False).wait_recv()

    for k in range(chunks):
        boxes_in = arrived[:, :, k * chunk : (k + 1) * chunk].astype(jnp.float32)
        boxes_in = boxes_in.reshape(boxes, chunk).astype(jnp.bfloat16)
        states[0, k] = jnp.dot(select[0], boxes_in, preferred_element_type=jnp.float32).astype(
            jnp.bfloat16
        )
        exchange(0, k).start()

    per_chunk = chunk // rows

    def weight(level, k, cols):
        piece = weights[level, k * per_chunk : (k + 1) * per_chunk, :, :, cols]
        return piece.reshape(chunk, chunk)

    for level in range(level_count):
        pumps(f"own{level}")
        flush(level)
        finish(level, 0, chunks * per_chunk)

        def own_part(n, carry):
            cols = pl.ds(pl.multiple_of(n * chunk, chunk), chunk)
            total = jnp.zeros((boxes, chunk), jnp.float32)
            for k in range(chunks):
                total += jnp.dot(
                    states[level, k], weight(level, k, cols), preferred_element_type=jnp.float32
                )
            acc[:, cols] = total
            return carry

        lax.fori_loop(0, chunks, own_part, 0)
        for k in range(chunks):
            pumps(f"level{level}.{k}")
            finish(level, (chunks + k) * per_chunk, per_chunk)
            exchange(level, k).wait_recv()
            aligned = jnp.dot(
                select[level + 1], partner[level, k], preferred_element_type=jnp.float32
            ).astype(jnp.bfloat16)
            if k < chunks - 1:

                def partner_part(n, carry):
                    cols = pl.ds(pl.multiple_of(n * chunk, chunk), chunk)
                    acc[:, cols] += jnp.dot(
                        aligned, weight(level, chunks + k, cols), preferred_element_type=jnp.float32
                    )
                    return carry

                lax.fori_loop(0, chunks, partner_part, 0)
            else:
                for n in range(chunks):
                    cols = pl.ds(n * chunk, chunk)
                    total = acc[:, cols] + jnp.dot(
                        aligned, weight(level, chunks + k, cols), preferred_element_type=jnp.float32
                    )
                    if level < level_count - 1:
                        states[level + 1, n] = total.astype(jnp.bfloat16)
                        exchange(level + 1, n).start()
                    else:
                        out[:, cols] = total.astype(jnp.bfloat16)

    for j in range(1, n_ta):
        for c in range(portions):
            regroup(j, c).wait_send()
    for offset in range(1, groups):
        moving(offset, True).wait_send()
    for level in range(level_count):
        for k in range(chunks):
            exchange(level, k).wait_send()
    for outer, condition, make in started:
        guarded(both(outer, condition), lambda: make().wait_send())


def on_device(sizes, traces, interp, translations, leaf_slot, pairing):
    n_gx, n_gy, n_ta = sizes
    groups = n_gx * n_gy
    boxes = leaf_slot.shape[0]
    levels, rows, width = translations.shape
    span = traces.shape[1]
    block = traces.shape[0] // n_ta
    chunk = max(TILE, rows)
    chunks = width // chunk
    table = jnp.asarray(spectrum_table(span * n_ta, NF))
    bf16, f32 = jnp.bfloat16, jnp.float32
    anywhere = pl.BlockSpec(memory_space=pl.ANY)
    vmem = pl.BlockSpec(memory_space=pltpu.VMEM)
    dma = pltpu.SemaphoreType.DMA
    return pl.pallas_call(
        functools.partial(kernel, sizes),
        out_shape=jax.ShapeDtypeStruct((boxes, width), bf16),
        in_specs=[anywhere, vmem, anywhere, vmem, vmem, anywhere],
        out_specs=vmem,
        scratch_shapes=[
            pltpu.VMEM((n_ta, block, span), bf16),
            pltpu.VMEM((levels, groups, 2, rows // 2, width), bf16),
            pltpu.VMEM((CHEB * BLOCK_BOXES, BLOCK_BOXES * BOXT), bf16),
            pltpu.VMEM((n_ta, CHEB, boxes, span), bf16),
            pltpu.VMEM((n_ta, CHEB, boxes, span), bf16),
            pltpu.VMEM(table.shape, bf16),
            pltpu.VMEM((boxes, width), f32),
            pltpu.VMEM((groups, boxes // groups, width), bf16),
            pltpu.VMEM((groups, boxes // groups, width), bf16),
            pltpu.VMEM((levels, chunks, boxes, chunk), bf16),
            pltpu.VMEM((levels, chunks, boxes, chunk), bf16),
            pltpu.VMEM((levels + 1, boxes, boxes), bf16),
            dma((n_ta,)),
            dma,
            dma((levels, 2)),
            dma((1,)),
            dma((levels, groups)),
            dma((levels, 2, groups)),
            dma((levels, max(1, n_gx.bit_length() - 1), groups)),
            dma((levels, groups)),
            dma((levels, groups)),
            dma((levels, 2, groups)),
            dma((levels, 2, groups)),
            dma((n_ta, min(4, groups))),
            dma((n_ta, min(4, groups))),
            dma((groups,)),
            dma((groups,)),
            dma((levels, chunks)),
            dma((levels, chunks)),
        ],
        compiler_params=pltpu.CompilerParams(
            collective_id=0, has_side_effects=True, vmem_limit_bytes=60 * 2**20
        ),
    )(traces, interp, translations, leaf_slot.reshape(1, boxes), pairing, table)


def solution(mesh):
    sizes = (mesh.shape["gx"], mesh.shape["gy"], mesh.shape["ta"])
    in_specs = (
        P(("gx", "gy"), "ta"),
        P(),
        P(None, ("gx", "gy"), None),
        P(("gx", "gy", "ta")),
        P(None, ("gx", "gy", "ta")),
    )
    out_specs = P(("gx", "gy", "ta"), None)
    return jax.shard_map(
        functools.partial(on_device, sizes),
        mesh=mesh,
        in_specs=in_specs,
        out_specs=out_specs,
        check_vma=False,
    )
```

```python
import functools
import math

import jax
import jax.numpy as jnp
import numpy as np
from jax import lax
from jax.experimental import pallas as pl
from jax.experimental.pallas import tpu as pltpu
from jax.sharding import PartitionSpec as P

NF = 256
CHEB = 2
BOXT = 16
BLOCK_BOXES = 16
TILE = 256
MESH = pl.DeviceIdType.MESH
KEPT = (0.625, 0.5, 0.75, 1)
SCHEDULE = {
    "start": ((1, 1, 1, 0), (0, 0, 0, -1),),
    "interp1": ((0, 1, 0, -1), (1, 2, 0, 2), (0, 0, 0, 0), (1, 1, 1, -1),),
    "table1": ((0, 0, 0, 2),),
    "spread1": ((1, 2, 1, -1), (0, 0, 1, -1),),
    "table2": ((0, 0, 1, 0),),
    "spread2": ((0, 0, 1, 2), (1, 2, 0, 1), (1, 1, 0, 1), (1, 0, 0, 2), (0, 0, 0, 1),),
    "table3": ((0, 1, 1, -1), (1, 1, 0, 0), (1, 3, 1, 2), (1, 1, 1, 2), (1, 3, 0, 2),),
    "spread3": (
        (0, 1, 0, 0),
        (0, 0, 1, 1),
        (0, 1, 0, 1),
        (1, 3, 0, 1),
        (0, 2, 0, -1),
        (1, 3, 1, 0),
        (1, 0, 0, 1),
        (1, 0, 1, 0),
    ),
    "spread": ((1, 0, 1, -1), (0, 1, 0, 2), (0, 3, 0, -1), (1, 0, 0, 0), (1, 0, 1, 1),),
    "own0": ((1, 2, 1, 0), (1, 0, 1, 2),),
    "level0.0": ((1, 2, 1, 1),),
    "level0.1": ((0, 2, 0, 0),),
    "level0.2": ((1, 3, 0, 0),),
    "level0.3": ((0, 1, 1, 0),),
    "own1": ((0, 2, 0, 1), (0, 1, 1, 1), (1, 1, 0, 2), (1, 1, 1, 1), (0, 1, 1, 2),),
    "level1.0": ((0, 2, 0, 2), (0, 3, 0, 0), (0, 2, 1, -1),),
    "level1.1": ((1, 3, 1, 1),),
    "level1.2": ((1, 2, 1, 2),),
    "own2": ((0, 2, 1, 0), (0, 3, 1, -1), (0, 3, 0, 1), (0, 2, 1, 1), (0, 2, 1, 2), (1, 2, 0, 0),),
    "level2.2": ((1, 3, 1, -1), (0, 3, 1, 0),),
    "own3": ((0, 3, 0, 2), (0, 3, 1, 2), (0, 3, 1, 1),),
}


def spectrum_table(length, count):
    sample_pos = np.arange(length, dtype=np.float32)[:, None]
    frequency = np.arange(count, dtype=np.float32)[None, :] + np.float32(1.0)
    angles = np.float32(2.0 * math.pi / length) * np.mod(sample_pos * frequency, np.float32(length))
    factor = np.float32(math.sqrt(2.0 / length))
    table = np.concatenate([np.cos(angles) * factor, -np.sin(angles) * factor], axis=1)
    return table.astype(jnp.bfloat16)


def flip(index, mask, size):
    result = index
    bit = 1
    while bit < size:
        if mask & bit:
            result = result + bit - 2 * bit * ((index // bit) % 2)
        bit *= 2
    return result


def mask_of(level, levels, devices):
    return 2 ** (level * (devices.bit_length() - 1) // levels)


def halves_join(sizes, levels, rows, width):
    n_gx, n_gy, n_ta = sizes
    devices = n_gx * n_gy * n_ta
    return (
        levels == 4
        and n_ta >= 4
        and mask_of(1, levels, devices) == 2
        and mask_of(2, levels, devices) >= n_ta
        and rows >= TILE
        and rows == max(TILE, rows)
        and width // rows >= 2
        and rows * n_gx * n_gy == 2 * width
    )


def kernel(
    sizes,
    traces,
    interp,
    translations,
    slots,
    pairs,
    table,
    out,
    tr,
    weights,
    mat,
    sampled,
    slices,
    fourier,
    acc,
    points,
    arrived,
    states,
    partner,
    select,
    narrow,
    short,
    pairs_twin,
    select_twin,
    turned,
    both_states,
    both_partner,
    sums,
    part_out,
    part_in,
    load_sem,
    table_sem,
    own_sem,
    ag_send,
    ag_recv,
    z_send,
    x_send,
    y_send,
    y_recv,
    core_send,
    core_recv,
    ta_send,
    ta_recv,
    g_send,
    g_recv,
    level_send,
    level_recv,
    pairs_sem,
    join_send,
    join_recv,
    part_send,
    part_recv,
):
    n_gx, n_gy, n_ta = sizes
    groups = n_gx * n_gy
    gx, gy, ta = lax.axis_index("gx"), lax.axis_index("gy"), lax.axis_index("ta")
    group = gx * n_gy + gy
    level_count = translations.shape[0]
    rows = translations.shape[1]
    half = rows // 2
    width = translations.shape[2]
    boxes = slots.shape[1]
    span = traces.shape[1]
    block = boxes * BOXT
    chunk = states.shape[3]
    chunks = width // chunk
    log_devices = (groups * n_ta).bit_length() - 1
    side = ta % 2

    def of_group(offset):
        p = flip(group, offset, groups)
        return (p // n_gy, p % n_gy, ta)

    def of_ta(offset):
        return (gx, gy, flip(ta, offset, n_ta))

    def loading(j):
        t = flip(ta, j, n_ta)
        return pltpu.make_async_copy(
            traces.at[pl.ds(pl.multiple_of(t * block, block), block), :], tr.at[j], load_sem.at[j]
        )

    upper = (ta // 2) % 2
    joined = halves_join(sizes, level_count, rows, width)

    def own(level):
        if joined and level == 1:
            strip = chunk // 2
            return [
                pltpu.make_async_copy(
                    translations.at[
                        level,
                        pl.ds(part * half, half),
                        pl.ds(pl.multiple_of(k * chunk + upper * strip, strip), strip),
                    ],
                    narrow.at[group, part, :, pl.ds(k * strip, strip)],
                    own_sem.at[level, part, k],
                )
                for part in range(2)
                for k in range(chunks)
            ]
        if joined and level == 2:
            quarter = half // 2
            return [
                pltpu.make_async_copy(
                    translations.at[
                        level,
                        pl.ds(pl.multiple_of(upper * half + part * quarter, quarter), quarter),
                        :,
                    ],
                    short.at[group, part],
                    own_sem.at[level, part, 0],
                )
                for part in range(2)
            ]
        return [
            pltpu.make_async_copy(
                translations.at[level, pl.ds(part * half, half), :],
                weights.at[level, group, part],
                own_sem.at[level, part, 0],
            )
            for part in range(2)
        ]

    xbits = []
    bit = n_gx // 2
    while bit:
        xbits.append(bit)
        bit //= 2
    stage_of = {0: -1}
    for stage, bit in enumerate(xbits):
        for offset in list(stage_of):
            stage_of[offset ^ bit] = stage
    lines = {offset: flip(gx, offset, n_gx) for offset in stage_of}
    shards = [
        (offset, d, k)
        for k in range(-1, n_gy - 1)
        for d in ((1,) if k < 0 else (1, -1))
        for offset in stage_of
    ]
    twins = n_ta >= 4
    twin = flip(ta, 2, n_ta) if twins else ta

    def kept(level):
        if not twins or (joined and level in (1, 2)):
            return half
        return max(half // 2, round(half * KEPT[level % len(KEPT)] / 16) * 16)

    def shard_id(offset, d, k):
        return lines[offset] * n_gy + gy - d * (k + 1)

    within = {
        (d, k): gy >= k + 1 if d > 0 else gy < n_gy - 1 - k
        for d in (1, -1)
        for k in range(n_gy - 1)
    }
    ahead = {1: gy < n_gy - 1, -1: gy > 0}

    def inside(d, k):
        return None if k < 0 else within[d, k]

    def both(a, b):
        if a is None or b is None:
            return b if a is None else a
        return jnp.logical_and(a, b)

    def guarded(condition, action):
        if condition is None:
            action()
        else:
            pl.when(condition)(action)

    started = []

    def launch(condition, make, outer=None):
        guarded(condition, lambda: make().start())
        started.append((outer, condition, make))

    def in_rows(level):
        size = kept(level)
        if size == half:
            return pl.ds(0, half)
        return pl.ds(pl.multiple_of(upper * (half - size), 16), size)

    def held(level, shard, part):
        if joined and level == 1:
            return narrow.at[shard, part]
        if joined and level == 2:
            return short.at[shard, part]
        return weights.at[level, shard, part, in_rows(level), :]

    def in_plane(level, shard, sem_ref, sem_at, target):
        place = held(level, shard, side)
        return pltpu.make_async_remote_copy(
            src_ref=place,
            dst_ref=place,
            send_sem=sem_ref.at[sem_at],
            recv_sem=ag_recv.at[level, shard],
            device_id=target,
            device_id_type=MESH,
        )

    def z_copy(level, shard, d):
        return in_plane(level, shard, z_send, (level, (d + 1) // 2, shard), (gx, gy + d, ta))

    def x_copy(level, shard, stage):
        target = (lines[xbits[stage]], gy, ta)
        return in_plane(level, shard, x_send, (level, stage, shard), target)

    def y_copy(level, shard, sending):
        size = kept(level)
        first = (upper if sending else 1 - upper) * size
        place = weights.at[level, shard, side, pl.ds(pl.multiple_of(first, 16), half - size), :]
        return pltpu.make_async_remote_copy(
            src_ref=place,
            dst_ref=place,
            send_sem=y_send.at[level, shard],
            recv_sem=y_recv.at[level, shard],
            device_id=(gx, gy, twin),
            device_id_type=MESH,
        )

    def core_copy(level, shard, kind, mine):
        size = kept(level)
        part = side if mine else 1 - side
        if kind == 0:
            place = held(level, shard, part)
        else:
            rows_at = pl.ds(pl.multiple_of((1 - upper) * size, 16), half - size)
            place = weights.at[level, shard, part, rows_at, :]
        return pltpu.make_async_remote_copy(
            src_ref=place,
            dst_ref=place,
            send_sem=core_send.at[level, kind, shard],
            recv_sem=core_recv.at[level, kind, shard],
            device_id=of_ta(1),
            device_id_type=MESH,
        )

    def has_twin(level):
        return kept(level) < half

    def forward(level, offset, d, k):
        shard = shard_id(offset, d, k)
        valid = inside(d, k)
        own_shard = offset == 0 and k < 0

        def body():
            if not own_shard:
                in_plane(level, shard, ag_send, 0, of_ta(1)).wait_recv()
                launch(None, lambda: core_copy(level, shard, 0, True), valid)
            if offset == 0:
                for way in (1, -1) if k < 0 else (d,):
                    launch(ahead[way], lambda way=way: z_copy(level, shard, way), valid)
            for stage in range(stage_of[offset] + 1, len(xbits)):
                launch(None, lambda stage=stage: x_copy(level, shard, stage), valid)
            if has_twin(level) and not own_shard:
                launch(None, lambda: y_copy(level, shard, True), valid)

        guarded(valid, body)

    def crossed(level, offset, d, k):
        shard = shard_id(offset, d, k)

        def body():
            y_copy(level, shard, False).wait_recv()
            launch(None, lambda: core_copy(level, shard, 1, True), inside(d, k))

        guarded(inside(d, k), body)

    handled = set()

    def piece(across, level, over, k):
        if (across, level, over, k) in handled or level >= level_count or k > n_gy - 2:
            return
        handled.add((across, level, over, k))
        if not (across or over) and k >= 0:
            piece(0, level, 0, k - 1)
        if across and not has_twin(level):
            return
        if k < 0 and not (across or over):
            for copy in own(level):
                copy.wait()
        for offset, d, at in shards:
            if at == k and (offset > 0) == (over > 0):
                if not across:
                    forward(level, offset, d, k)
                elif offset or k >= 0:
                    crossed(level, offset, d, k)

    def pumps(point):
        for entry in SCHEDULE.get(point, ()):
            piece(*entry)

    def flush(level):
        for across in range(2):
            for total in range(-1, n_gy):
                for over in range(2):
                    if -1 <= total - over < n_gy - 1:
                        piece(across, level, over, total - over)

    def finish(level, first, count):
        for shard in range(first, first + count):

            def body():
                core_copy(level, shard, 0, False).wait_recv()
                if has_twin(level):
                    core_copy(level, shard, 1, False).wait_recv()

            pl.when(group != shard)(body)

    portions = min(4, groups)
    per_portion = groups // portions
    portion_rows = boxes // portions
    portion_order = sorted(range(portions), key=lambda c: (-(c % 2), -c))

    def portion(c):
        return flip(group // per_portion, c, portions)

    def portion_at(c):
        return pl.multiple_of(portion(c) * portion_rows, portion_rows)

    def regroup(j, c):
        place = pl.ds(portion_at(c), portion_rows)
        return pltpu.make_async_remote_copy(
            src_ref=sampled.at[j, :, place, :],
            dst_ref=slices.at[j, :, place, :],
            send_sem=ta_send.at[j, c],
            recv_sem=ta_recv.at[j, c],
            device_id=of_ta(j),
            device_id_type=MESH,
        )

    def moving(offset, sending):
        src = points.at[flip(group, offset, groups)]
        dst = arrived.at[group if sending else flip(group, offset, groups)]
        return pltpu.make_async_remote_copy(
            src_ref=src,
            dst_ref=dst,
            send_sem=g_send.at[offset],
            recv_sem=g_recv.at[offset],
            device_id=of_group(offset),
            device_id_type=MESH,
        )

    def exchange(level, k):
        mask = 2 ** (level * log_devices // level_count)
        target = of_ta(mask) if mask < n_ta else of_group(mask // n_ta)
        return pltpu.make_async_remote_copy(
            src_ref=states.at[level, k],
            dst_ref=partner.at[level, k],
            send_sem=level_send.at[level, k],
            recv_sem=level_recv.at[level, k],
            device_id=target,
            device_id_type=MESH,
        )

    def twin_copy(src, dst, sems):
        return pltpu.make_async_remote_copy(
            src_ref=src,
            dst_ref=dst,
            send_sem=sems[0],
            recv_sem=sems[1],
            device_id=of_ta(2),
            device_id_type=MESH,
        )

    def pairs_copy():
        return twin_copy(pairs, pairs_twin, (pairs_sem.at[0], pairs_sem.at[1]))

    def handing(n):
        return twin_copy(part_out.at[n], part_in.at[n], (part_send.at[n], part_recv.at[n]))

    def join(r, n):
        return pltpu.make_async_remote_copy(
            src_ref=both_states.at[r, n],
            dst_ref=both_partner.at[r, n],
            send_sem=join_send.at[r, n],
            recv_sem=join_recv.at[r, n],
            device_id=of_group(mask_of(2, level_count, groups * n_ta) // n_ta),
            device_id_type=MESH,
        )

    near = [n_ta - 1 - j for j in range(n_ta)]
    for j in near:
        loading(j).start()
    for level in range(level_count):
        for copy in own(level):
            copy.start()
    table_copy = pltpu.make_async_copy(table, fourier, table_sem)
    table_copy.start()

    barrier = pltpu.get_barrier_semaphore()
    for j in range(1, n_ta):
        pl.semaphore_signal(barrier, inc=1, device_id=of_ta(j), device_id_type=MESH)
    for offset in range(1, groups):
        pl.semaphore_signal(barrier, inc=1, device_id=of_group(offset), device_id_type=MESH)

    columns = BLOCK_BOXES * BOXT
    spread = (
        lax.broadcasted_iota(jnp.int32, (BOXT, columns), 1) % BOXT
        == lax.broadcasted_iota(jnp.int32, (BOXT, columns), 0)
    )
    tiled = jnp.dot(
        interp[...], spread.astype(jnp.float32).astype(jnp.bfloat16), preferred_element_type=jnp.float32
    )
    own_box = (
        lax.broadcasted_iota(jnp.int32, (BLOCK_BOXES, columns), 1) // BOXT
        == lax.broadcasted_iota(jnp.int32, (BLOCK_BOXES, columns), 0)
    )
    for c in range(CHEB):
        mat[pl.ds(c * BLOCK_BOXES, BLOCK_BOXES), :] = jnp.where(
            own_box, tiled[c : c + 1, :], 0.0
        ).astype(jnp.bfloat16)

    def selection(index_row):
        hit = lax.broadcasted_iota(jnp.int32, (boxes, boxes), 0) == index_row
        return jnp.where(hit, 1.0, 0.0).T.astype(jnp.bfloat16)

    select[0] = selection(slots[...])
    for level in range(level_count):
        select[level + 1] = selection(pairs[pl.ds(level, 1), :])

    pl.semaphore_wait(barrier, n_ta - 1 + groups - 1)
    pumps("start")
    if joined:
        pairs_copy().start()

    for turn, c in enumerate(portion_order):
        for j in near:
            if turn == 0:
                loading(j).wait()
            where = sampled if j else slices
            for i in range(portion_rows // BLOCK_BOXES):
                box = pl.multiple_of(portion_at(c) + i * BLOCK_BOXES, BLOCK_BOXES)
                traces_block = tr[j, pl.ds(pl.multiple_of(box * BOXT, columns), columns), :]
                pair = jnp.dot(mat[...], traces_block, preferred_element_type=jnp.float32)
                pair = pair.astype(jnp.bfloat16)
                for q in range(CHEB):
                    where[j, q, pl.ds(box, BLOCK_BOXES), :] = pair[
                        q * BLOCK_BOXES : (q + 1) * BLOCK_BOXES, :
                    ]
            if j:
                regroup(j, c).start()
        pumps(f"interp{turn}")

    table_copy.wait()
    for turn, c in enumerate(portion_order):
        pumps(f"table{turn}")
        place = pl.ds(portion_at(c), portion_rows)
        total = jnp.zeros((CHEB * portion_rows, 2 * NF), jnp.float32)
        for j in range(n_ta):
            if j:
                regroup(j, c).wait_recv()
            first = pl.multiple_of(flip(ta, j, n_ta) * span, span)
            part = slices[j, :, place, :].reshape(CHEB * portion_rows, span)
            total += jnp.dot(part, fourier[pl.ds(first, span), :], preferred_element_type=jnp.float32)
        mine = pl.ds(portion(c) * per_portion, per_portion)
        for q in range(CHEB):
            points[mine, :, q * 2 * NF : (q + 1) * 2 * NF] = (
                total[q * portion_rows : (q + 1) * portion_rows, :]
                .reshape(per_portion, boxes // groups, 2 * NF)
                .astype(jnp.bfloat16)
            )
        for offset in range((c + 1) * per_portion - 1, c * per_portion - 1, -1):
            if offset:
                moving(offset, True).start()
        pumps(f"spread{turn}")
    arrived[group] = points[group]
    if joined:
        pairs_copy().wait_recv()
        for level in (1, 2):
            select_twin[level - 1] = selection(pairs_twin[pl.ds(level, 1), :])
    pumps("spread")
    for offset in range(1, groups):
        moving(offset, False).wait_recv()

    for k in range(chunks):
        boxes_in = arrived[:, :, k * chunk : (k + 1) * chunk].astype(jnp.float32)
        boxes_in = boxes_in.reshape(boxes, chunk).astype(jnp.bfloat16)
        states[0, k] = jnp.dot(select[0], boxes_in, preferred_element_type=jnp.float32).astype(
            jnp.bfloat16
        )
        exchange(0, k).start()

    per_chunk = chunk // rows

    def weight(level, k, cols):
        piece = weights[level, k * per_chunk : (k + 1) * per_chunk, :, :, cols]
        return piece.reshape(chunk, chunk)

    def dots(left, right):
        return jnp.dot(left, right, preferred_element_type=jnp.float32)

    def columns_of(n):
        return pl.ds(pl.multiple_of(n * chunk, chunk), chunk)

    def first_joined(level):
        pumps(f"own{level}")
        flush(level)
        finish(level, 0, 2 * chunks * per_chunk)

        def piece_of(k, cols):
            return narrow[k, :, :, cols].reshape(chunk, chunk)

        for k in range(chunks):
            turned[k] = dots(select_twin[level - 1], states[level, k]).astype(jnp.bfloat16)

        def own_part(n, carry):
            cols = columns_of(n)
            straight = jnp.zeros((boxes, chunk), jnp.float32)
            for k in range(chunks):
                straight += dots(states[level, k], piece_of(k, cols))
            sums[0, :, cols] = straight
            across = jnp.zeros((boxes, chunk), jnp.float32)
            for k in range(chunks):
                across += dots(turned[k], piece_of(chunks + k, cols))
            sums[1, :, cols] = across
            return carry

        lax.fori_loop(0, chunks // 2, own_part, 0)
        for k in range(chunks):
            pumps(f"level{level}.{k}")
            exchange(level, k).wait_recv()
            aligned = dots(select[level + 1], partner[level, k]).astype(jnp.bfloat16)
            if k < chunks - 1:

                def partner_part(n, carry):
                    cols = columns_of(n)
                    sums[1, :, cols] += dots(partner[level, k], piece_of(k, cols))
                    sums[0, :, cols] += dots(aligned, piece_of(chunks + k, cols))
                    return carry

                lax.fori_loop(0, chunks // 2, partner_part, 0)
            else:
                for r in (1, 0):
                    for n in range(chunks // 2):
                        cols = pl.ds(n * chunk, chunk)
                        if r:
                            last = dots(partner[level, k], piece_of(k, cols))
                        else:
                            last = dots(aligned, piece_of(chunks + k, cols))
                        both_states[r, n] = (sums[r, :, cols] + last).astype(jnp.bfloat16)
                        join(r, n).start()

    def second_joined(level):
        pumps(f"own{level}")
        flush(level)
        finish(level, 0, 2 * chunks * per_chunk)

        def piece_of(n, cols):
            return short[2 * n : 2 * n + 2, :, :, cols].reshape(chunk, chunk)

        for r in (1, 0):

            def own_part(q, carry):
                cols = columns_of(q)
                total = jnp.zeros((boxes, chunk), jnp.float32)
                for n in range(chunks // 2):
                    total += dots(both_states[r, n], piece_of(n, cols))
                sums[r, :, cols] = total
                return carry

            lax.fori_loop(0, chunks, own_part, 0)
        turns = [(r, n) for r in (1, 0) for n in range(chunks // 2)]
        for turn, (r, n) in enumerate(turns):
            if turn < chunks:
                pumps(f"level{level}.{turn}")
            join(r, n).wait_recv()
            table_of = select_twin[level - 1] if r else select[level + 1]
            aligned = dots(table_of, both_partner[r, n]).astype(jnp.bfloat16)
            if n < chunks // 2 - 1:

                def partner_part(q, carry):
                    cols = columns_of(q)
                    sums[r, :, cols] += dots(aligned, piece_of(chunks // 2 + n, cols))
                    return carry

                lax.fori_loop(0, chunks, partner_part, 0)
                continue
            for q in range(chunks):
                cols = pl.ds(q * chunk, chunk)
                total = sums[r, :, cols] + dots(aligned, piece_of(chunks // 2 + n, cols))
                if r:
                    part_out[q] = total.astype(jnp.bfloat16)
                    handing(q).start()
                else:
                    handing(q).wait_recv()
                    total += part_in[q].astype(jnp.float32)
                    states[level + 1, q] = total.astype(jnp.bfloat16)
                    exchange(level + 1, q).start()

    def plain_level(level):
        pumps(f"own{level}")
        flush(level)
        finish(level, 0, chunks * per_chunk)

        def own_part(n, carry):
            cols = pl.ds(pl.multiple_of(n * chunk, chunk), chunk)
            total = jnp.zeros((boxes, chunk), jnp.float32)
            for k in range(chunks):
                total += jnp.dot(
                    states[level, k], weight(level, k, cols), preferred_element_type=jnp.float32
                )
            acc[:, cols] = total
            return carry

        lax.fori_loop(0, chunks, own_part, 0)
        for k in range(chunks):
            pumps(f"level{level}.{k}")
            finish(level, (chunks + k) * per_chunk, per_chunk)
            exchange(level, k).wait_recv()
            aligned = jnp.dot(
                select[level + 1], partner[level, k], preferred_element_type=jnp.float32
            ).astype(jnp.bfloat16)
            if k < chunks - 1:

                def partner_part(n, carry):
                    cols = pl.ds(pl.multiple_of(n * chunk, chunk), chunk)
                    acc[:, cols] += jnp.dot(
                        aligned, weight(level, chunks + k, cols), preferred_element_type=jnp.float32
                    )
                    return carry

                lax.fori_loop(0, chunks, partner_part, 0)
            else:
                for n in range(chunks):
                    cols = pl.ds(n * chunk, chunk)
                    total = acc[:, cols] + jnp.dot(
                        aligned, weight(level, chunks + k, cols), preferred_element_type=jnp.float32
                    )
                    if level < level_count - 1:
                        states[level + 1, n] = total.astype(jnp.bfloat16)
                        exchange(level + 1, n).start()
                    else:
                        out[:, cols] = total.astype(jnp.bfloat16)

    for level in range(level_count):
        if joined and level in (1, 2):
            (first_joined if level == 1 else second_joined)(level)
        else:
            plain_level(level)

    for j in range(1, n_ta):
        for c in range(portions):
            regroup(j, c).wait_send()
    for offset in range(1, groups):
        moving(offset, True).wait_send()
    for level in range(level_count):
        for k in range(chunks):
            if not (joined and level == 2):
                exchange(level, k).wait_send()
    if joined:
        pairs_copy().wait_send()
        for n in range(chunks):
            handing(n).wait_send()
        for r in range(2):
            for n in range(chunks // 2):
                join(r, n).wait_send()
    for outer, condition, make in started:
        guarded(both(outer, condition), lambda: make().wait_send())


def on_device(sizes, traces, interp, translations, leaf_slot, pairing):
    n_gx, n_gy, n_ta = sizes
    groups = n_gx * n_gy
    boxes = leaf_slot.shape[0]
    levels, rows, width = translations.shape
    span = traces.shape[1]
    block = traces.shape[0] // n_ta
    chunk = max(TILE, rows)
    chunks = width // chunk
    table = jnp.asarray(spectrum_table(span * n_ta, NF))
    bf16, f32 = jnp.bfloat16, jnp.float32
    joined = halves_join(sizes, levels, rows, width)

    def extra(shape, kind):
        return pltpu.VMEM(shape if joined else (1,) * (len(shape) - 2) + (16, 128), kind)

    anywhere = pl.BlockSpec(memory_space=pl.ANY)
    vmem = pl.BlockSpec(memory_space=pltpu.VMEM)
    dma = pltpu.SemaphoreType.DMA
    return pl.pallas_call(
        functools.partial(kernel, sizes),
        out_shape=jax.ShapeDtypeStruct((boxes, width), bf16),
        in_specs=[anywhere, vmem, anywhere, vmem, vmem, anywhere],
        out_specs=vmem,
        scratch_shapes=[
            pltpu.VMEM((n_ta, block, span), bf16),
            pltpu.VMEM((levels, groups, 2, rows // 2, width), bf16),
            pltpu.VMEM((CHEB * BLOCK_BOXES, BLOCK_BOXES * BOXT), bf16),
            pltpu.VMEM((n_ta, CHEB, boxes, span), bf16),
            pltpu.VMEM((n_ta, CHEB, boxes, span), bf16),
            pltpu.VMEM(table.shape, bf16),
            pltpu.VMEM((boxes, width), f32),
            pltpu.VMEM((groups, boxes // groups, width), bf16),
            pltpu.VMEM((groups, boxes // groups, width), bf16),
            pltpu.VMEM((levels, chunks, boxes, chunk), bf16),
            pltpu.VMEM((levels, chunks, boxes, chunk), bf16),
            pltpu.VMEM((levels + 1, boxes, boxes), bf16),
            extra((groups, 2, rows // 2, width // 2), bf16),
            extra((groups, 2, rows // 4, width), bf16),
            extra((levels, boxes), jnp.int32),
            extra((2, boxes, boxes), bf16),
            extra((chunks, boxes, chunk), bf16),
            extra((2, chunks // 2, boxes, chunk), bf16),
            extra((2, chunks // 2, boxes, chunk), bf16),
            extra((2, boxes, width), f32),
            extra((chunks, boxes, chunk), bf16),
            extra((chunks, boxes, chunk), bf16),
            dma((n_ta,)),
            dma,
            dma((levels, 2, chunks)),
            dma((1,)),
            dma((levels, groups)),
            dma((levels, 2, groups)),
            dma((levels, max(1, n_gx.bit_length() - 1), groups)),
            dma((levels, groups)),
            dma((levels, groups)),
            dma((levels, 2, groups)),
            dma((levels, 2, groups)),
            dma((n_ta, min(4, groups))),
            dma((n_ta, min(4, groups))),
            dma((groups,)),
            dma((groups,)),
            dma((levels, chunks)),
            dma((levels, chunks)),
            dma((2,)),
            dma((2, max(1, chunks // 2))),
            dma((2, max(1, chunks // 2))),
            dma((chunks,)),
            dma((chunks,)),
        ],
        compiler_params=pltpu.CompilerParams(
            collective_id=0, has_side_effects=True, vmem_limit_bytes=60 * 2**20
        ),
    )(traces, interp, translations, leaf_slot.reshape(1, boxes), pairing, table)


def solution(mesh):
    sizes = (mesh.shape["gx"], mesh.shape["gy"], mesh.shape["ta"])
    in_specs = (
        P(("gx", "gy"), "ta"),
        P(),
        P(None, ("gx", "gy"), None),
        P(("gx", "gy", "ta")),
        P(None, ("gx", "gy", "ta")),
    )
    out_specs = P(("gx", "gy", "ta"), None)
    return jax.shard_map(
        functools.partial(on_device, sizes),
        mesh=mesh,
        in_specs=in_specs,
        out_specs=out_specs,
        check_vma=False,
    )
```

```python
import functools
import math

import jax
import jax.numpy as jnp
import numpy as np
from jax import lax
from jax.experimental import pallas as pl
from jax.experimental.pallas import tpu as pltpu
from jax.sharding import PartitionSpec as P

NF = 256
CHEB = 2
BOXT = 16
BLOCK_BOXES = 16
TILE = 256
MESH = pl.DeviceIdType.MESH
KEPT = (0.625, 0.5, 0.625, 1)
SCHEDULE = {
    "start": ((1, 1, 0, 1), (0, 0, 0, -1),),
    "interp0": ((1, 1, 1, 1),),
    "interp1": ((0, 1, 0, -1),),
    "interp3": ((0, 0, 1, -1), (1, 1, 0, 0), (0, 0, 0, 0), (1, 1, 1, -1),),
    "spread0": ((1, 1, 0, 2), (0, 0, 0, 1), (1, 2, 0, 2), (1, 1, 1, 0),),
    "table1": ((1, 0, 1, -1),),
    "spread1": ((1, 2, 1, 0), (0, 0, 0, 2), (1, 3, 1, 2),),
    "table2": ((1, 2, 1, -1), (0, 0, 1, 0),),
    "spread2": ((0, 0, 1, 2), (0, 1, 1, -1), (0, 1, 0, 0),),
    "table3": ((1, 0, 0, 1), (1, 0, 0, 0), (1, 3, 0, 1), (1, 3, 1, 1),),
    "spread3": (
        (0, 0, 1, 1),
        (1, 0, 0, 2),
        (0, 2, 0, -1),
        (1, 0, 1, 0),
        (1, 0, 1, 2),
        (0, 1, 0, 1),
        (1, 0, 1, 1),
    ),
    "level0.0": ((0, 1, 0, 2), (1, 2, 0, 0), (0, 2, 0, 0), (1, 2, 1, 2),),
    "level0.2": ((0, 3, 0, -1),),
    "own1": (
        (0, 2, 1, -1),
        (0, 1, 1, 2),
        (1, 1, 1, 2),
        (0, 2, 0, 1),
        (0, 1, 1, 1),
        (0, 1, 1, 0),
        (1, 2, 1, 1),
        (0, 2, 0, 2),
        (1, 2, 0, 1),
        (0, 3, 0, 0),
    ),
    "own2": ((0, 2, 1, 0), (1, 3, 0, 2), (0, 2, 1, 1), (0, 2, 1, 2), (0, 3, 0, 1),),
    "level2.0": ((1, 3, 1, 0),),
    "level2.1": ((1, 3, 1, -1),),
    "level2.2": ((1, 3, 0, 0), (0, 3, 1, 0),),
    "own3": ((0, 3, 1, 1), (0, 3, 0, 2), (0, 3, 1, 2), (0, 3, 1, -1),),
}


def spectrum_table(length, count):
    sample_pos = np.arange(length, dtype=np.float32)[:, None]
    frequency = np.arange(count, dtype=np.float32)[None, :] + np.float32(1.0)
    angles = np.float32(2.0 * math.pi / length) * np.mod(sample_pos * frequency, np.float32(length))
    factor = np.float32(math.sqrt(2.0 / length))
    table = np.concatenate([np.cos(angles) * factor, -np.sin(angles) * factor], axis=1)
    return table.astype(jnp.bfloat16)


def flip(index, mask, size):
    result = index
    bit = 1
    while bit < size:
        if mask & bit:
            result = result + bit - 2 * bit * ((index // bit) % 2)
        bit *= 2
    return result


def mask_of(level, levels, devices):
    return 2 ** (level * (devices.bit_length() - 1) // levels)


def halves_join(sizes, levels, rows, width):
    n_gx, n_gy, n_ta = sizes
    devices = n_gx * n_gy * n_ta
    return (
        levels == 4
        and n_ta >= 4
        and mask_of(1, levels, devices) == 2
        and mask_of(2, levels, devices) >= n_ta
        and rows >= TILE
        and rows == max(TILE, rows)
        and width // rows >= 2
        and rows * n_gx * n_gy == 2 * width
    )


def kernel(
    sizes,
    traces,
    interp,
    translations,
    slots,
    pairs,
    table,
    out,
    tr,
    weights,
    mat,
    sampled,
    slices,
    fourier,
    acc,
    points,
    arrived,
    states,
    partner,
    select,
    narrow,
    short,
    pairs_twin,
    select_twin,
    turned,
    both_states,
    both_partner,
    sums,
    part_out,
    part_in,
    load_sem,
    table_sem,
    own_sem,
    ag_send,
    ag_recv,
    z_send,
    x_send,
    y_send,
    y_recv,
    core_send,
    core_recv,
    ta_send,
    ta_recv,
    g_send,
    g_recv,
    level_send,
    level_recv,
    pairs_sem,
    join_send,
    join_recv,
    part_send,
    part_recv,
):
    n_gx, n_gy, n_ta = sizes
    groups = n_gx * n_gy
    gx, gy, ta = lax.axis_index("gx"), lax.axis_index("gy"), lax.axis_index("ta")
    group = gx * n_gy + gy
    level_count = translations.shape[0]
    rows = translations.shape[1]
    half = rows // 2
    width = translations.shape[2]
    boxes = slots.shape[1]
    span = traces.shape[1]
    block = boxes * BOXT
    chunk = states.shape[3]
    chunks = width // chunk
    log_devices = (groups * n_ta).bit_length() - 1
    side = ta % 2

    def of_group(offset):
        p = flip(group, offset, groups)
        return (p // n_gy, p % n_gy, ta)

    def of_ta(offset):
        return (gx, gy, flip(ta, offset, n_ta))

    upper = (ta // 2) % 2
    joined = halves_join(sizes, level_count, rows, width)

    def own(level):
        if joined and level == 1:
            strip = chunk // 2
            return [
                pltpu.make_async_copy(
                    translations.at[
                        level,
                        pl.ds(part * half, half),
                        pl.ds(pl.multiple_of(k * chunk + upper * strip, strip), strip),
                    ],
                    narrow.at[group, part, :, pl.ds(k * strip, strip)],
                    own_sem.at[level, part, k],
                )
                for part in range(2)
                for k in range(chunks)
            ]
        if joined and level == 2:
            quarter = half // 2
            return [
                pltpu.make_async_copy(
                    translations.at[
                        level,
                        pl.ds(pl.multiple_of(upper * half + part * quarter, quarter), quarter),
                        :,
                    ],
                    short.at[group, part],
                    own_sem.at[level, part, 0],
                )
                for part in range(2)
            ]
        return [
            pltpu.make_async_copy(
                translations.at[level, pl.ds(part * half, half), :],
                weights.at[level, group, part],
                own_sem.at[level, part, 0],
            )
            for part in range(2)
        ]

    xbits = []
    bit = n_gx // 2
    while bit:
        xbits.append(bit)
        bit //= 2
    stage_of = {0: -1}
    for stage, bit in enumerate(xbits):
        for offset in list(stage_of):
            stage_of[offset ^ bit] = stage
    lines = {offset: flip(gx, offset, n_gx) for offset in stage_of}
    shards = [
        (offset, d, k)
        for k in range(-1, n_gy - 1)
        for d in ((1,) if k < 0 else (1, -1))
        for offset in stage_of
    ]
    twins = n_ta >= 4
    twin = flip(ta, 2, n_ta) if twins else ta

    def kept(level):
        if not twins or (joined and level in (1, 2)):
            return half
        return max(half // 2, round(half * KEPT[level % len(KEPT)] / 16) * 16)

    def shard_id(offset, d, k):
        return lines[offset] * n_gy + gy - d * (k + 1)

    within = {
        (d, k): gy >= k + 1 if d > 0 else gy < n_gy - 1 - k
        for d in (1, -1)
        for k in range(n_gy - 1)
    }
    ahead = {1: gy < n_gy - 1, -1: gy > 0}

    def inside(d, k):
        return None if k < 0 else within[d, k]

    def both(a, b):
        if a is None or b is None:
            return b if a is None else a
        return jnp.logical_and(a, b)

    def guarded(condition, action):
        if condition is None:
            action()
        else:
            pl.when(condition)(action)

    started = []

    def launch(condition, make, outer=None):
        guarded(condition, lambda: make().start())
        started.append((outer, condition, make))

    def in_rows(level):
        size = kept(level)
        if size == half:
            return pl.ds(0, half)
        return pl.ds(pl.multiple_of(upper * (half - size), 16), size)

    def held(level, shard, part):
        if joined and level == 1:
            return narrow.at[shard, part]
        if joined and level == 2:
            return short.at[shard, part]
        return weights.at[level, shard, part, in_rows(level), :]

    def in_plane(level, shard, sem_ref, sem_at, target):
        place = held(level, shard, side)
        return pltpu.make_async_remote_copy(
            src_ref=place,
            dst_ref=place,
            send_sem=sem_ref.at[sem_at],
            recv_sem=ag_recv.at[level, shard],
            device_id=target,
            device_id_type=MESH,
        )

    def z_copy(level, shard, d):
        return in_plane(level, shard, z_send, (level, (d + 1) // 2, shard), (gx, gy + d, ta))

    def x_copy(level, shard, stage):
        target = (lines[xbits[stage]], gy, ta)
        return in_plane(level, shard, x_send, (level, stage, shard), target)

    def y_copy(level, shard, sending):
        size = kept(level)
        first = (upper if sending else 1 - upper) * size
        place = weights.at[level, shard, side, pl.ds(pl.multiple_of(first, 16), half - size), :]
        return pltpu.make_async_remote_copy(
            src_ref=place,
            dst_ref=place,
            send_sem=y_send.at[level, shard],
            recv_sem=y_recv.at[level, shard],
            device_id=(gx, gy, twin),
            device_id_type=MESH,
        )

    def core_copy(level, shard, kind, mine):
        size = kept(level)
        part = side if mine else 1 - side
        if kind == 0:
            place = held(level, shard, part)
        else:
            rows_at = pl.ds(pl.multiple_of((1 - upper) * size, 16), half - size)
            place = weights.at[level, shard, part, rows_at, :]
        return pltpu.make_async_remote_copy(
            src_ref=place,
            dst_ref=place,
            send_sem=core_send.at[level, kind, shard],
            recv_sem=core_recv.at[level, kind, shard],
            device_id=of_ta(1),
            device_id_type=MESH,
        )

    def has_twin(level):
        return kept(level) < half

    def forward(level, offset, d, k):
        shard = shard_id(offset, d, k)
        valid = inside(d, k)
        own_shard = offset == 0 and k < 0

        def body():
            if not own_shard:
                in_plane(level, shard, ag_send, 0, of_ta(1)).wait_recv()
                launch(None, lambda: core_copy(level, shard, 0, True), valid)
            if offset == 0:
                for way in (1, -1) if k < 0 else (d,):
                    launch(ahead[way], lambda way=way: z_copy(level, shard, way), valid)
            for stage in range(stage_of[offset] + 1, len(xbits)):
                launch(None, lambda stage=stage: x_copy(level, shard, stage), valid)
            if has_twin(level) and not own_shard:
                launch(None, lambda: y_copy(level, shard, True), valid)

        guarded(valid, body)

    def crossed(level, offset, d, k):
        shard = shard_id(offset, d, k)

        def body():
            y_copy(level, shard, False).wait_recv()
            launch(None, lambda: core_copy(level, shard, 1, True), inside(d, k))

        guarded(inside(d, k), body)

    handled = set()

    def piece(across, level, over, k):
        if (across, level, over, k) in handled or level >= level_count or k > n_gy - 2:
            return
        handled.add((across, level, over, k))
        if not (across or over) and k >= 0:
            piece(0, level, 0, k - 1)
        if across and not has_twin(level):
            return
        if k < 0 and not (across or over):
            for copy in own(level):
                copy.wait()
        for offset, d, at in shards:
            if at == k and (offset > 0) == (over > 0):
                if not across:
                    forward(level, offset, d, k)
                elif offset or k >= 0:
                    crossed(level, offset, d, k)

    def pumps(point):
        for entry in SCHEDULE.get(point, ()):
            piece(*entry)

    def flush(level):
        for across in range(2):
            for total in range(-1, n_gy):
                for over in range(2):
                    if -1 <= total - over < n_gy - 1:
                        piece(across, level, over, total - over)

    def finish(level, first, count):
        for shard in range(first, first + count):

            def body():
                core_copy(level, shard, 0, False).wait_recv()
                if has_twin(level):
                    core_copy(level, shard, 1, False).wait_recv()

            pl.when(group != shard)(body)

    portions = min(4, groups)
    per_portion = groups // portions
    portion_rows = boxes // portions
    portion_order = sorted(range(portions), key=lambda c: (-(c % 2), -c))

    def portion(c):
        return flip(group // per_portion, c, portions)

    def portion_at(c):
        return pl.multiple_of(portion(c) * portion_rows, portion_rows)

    def loading(j, c):
        size = portion_rows * BOXT
        first = pl.multiple_of(portion(c) * size, size)
        source = pl.multiple_of(flip(ta, j, n_ta) * block + first, size)
        return pltpu.make_async_copy(
            traces.at[pl.ds(source, size), :], tr.at[j, pl.ds(first, size), :], load_sem.at[j, c]
        )

    def regroup(j, c):
        place = pl.ds(portion_at(c), portion_rows)
        return pltpu.make_async_remote_copy(
            src_ref=sampled.at[j, :, place, :],
            dst_ref=slices.at[j, :, place, :],
            send_sem=ta_send.at[j, c],
            recv_sem=ta_recv.at[j, c],
            device_id=of_ta(j),
            device_id_type=MESH,
        )

    def moving(offset, sending):
        src = points.at[flip(group, offset, groups)]
        dst = arrived.at[group if sending else flip(group, offset, groups)]
        return pltpu.make_async_remote_copy(
            src_ref=src,
            dst_ref=dst,
            send_sem=g_send.at[offset],
            recv_sem=g_recv.at[offset],
            device_id=of_group(offset),
            device_id_type=MESH,
        )

    def exchange(level, k):
        mask = 2 ** (level * log_devices // level_count)
        target = of_ta(mask) if mask < n_ta else of_group(mask // n_ta)
        return pltpu.make_async_remote_copy(
            src_ref=states.at[level, k],
            dst_ref=partner.at[level, k],
            send_sem=level_send.at[level, k],
            recv_sem=level_recv.at[level, k],
            device_id=target,
            device_id_type=MESH,
        )

    def twin_copy(src, dst, sems):
        return pltpu.make_async_remote_copy(
            src_ref=src,
            dst_ref=dst,
            send_sem=sems[0],
            recv_sem=sems[1],
            device_id=of_ta(2),
            device_id_type=MESH,
        )

    def pairs_copy():
        return twin_copy(pairs, pairs_twin, (pairs_sem.at[0], pairs_sem.at[1]))

    def handing(n):
        return twin_copy(part_out.at[n], part_in.at[n], (part_send.at[n], part_recv.at[n]))

    def join(r, n):
        return pltpu.make_async_remote_copy(
            src_ref=both_states.at[r, n],
            dst_ref=both_partner.at[r, n],
            send_sem=join_send.at[r, n],
            recv_sem=join_recv.at[r, n],
            device_id=of_group(mask_of(2, level_count, groups * n_ta) // n_ta),
            device_id_type=MESH,
        )

    near = [n_ta - 1 - j for j in range(n_ta)]
    table_copy = pltpu.make_async_copy(table, fourier, table_sem)
    for copy in own(0):
        copy.start()
    for turn, c in enumerate(portion_order):
        for j in near:
            loading(j, c).start()
        if turn == 0:
            table_copy.start()
            for copy in own(1):
                copy.start()
    for level in range(2, level_count):
        for copy in own(level):
            copy.start()

    barrier = pltpu.get_barrier_semaphore()
    for j in range(1, n_ta):
        pl.semaphore_signal(barrier, inc=1, device_id=of_ta(j), device_id_type=MESH)
    for offset in range(1, groups):
        pl.semaphore_signal(barrier, inc=1, device_id=of_group(offset), device_id_type=MESH)

    columns = BLOCK_BOXES * BOXT
    spread = (
        lax.broadcasted_iota(jnp.int32, (BOXT, columns), 1) % BOXT
        == lax.broadcasted_iota(jnp.int32, (BOXT, columns), 0)
    )
    tiled = jnp.dot(
        interp[...], spread.astype(jnp.float32).astype(jnp.bfloat16), preferred_element_type=jnp.float32
    )
    own_box = (
        lax.broadcasted_iota(jnp.int32, (BLOCK_BOXES, columns), 1) // BOXT
        == lax.broadcasted_iota(jnp.int32, (BLOCK_BOXES, columns), 0)
    )
    for c in range(CHEB):
        mat[pl.ds(c * BLOCK_BOXES, BLOCK_BOXES), :] = jnp.where(
            own_box, tiled[c : c + 1, :], 0.0
        ).astype(jnp.bfloat16)

    def selection(index_row):
        hit = lax.broadcasted_iota(jnp.int32, (boxes, boxes), 0) == index_row
        return jnp.where(hit, 1.0, 0.0).T.astype(jnp.bfloat16)

    select[0] = selection(slots[...])
    for level in range(level_count):
        select[level + 1] = selection(pairs[pl.ds(level, 1), :])

    pl.semaphore_wait(barrier, n_ta - 1 + groups - 1)
    pumps("start")
    if joined:
        pairs_copy().start()

    for turn, c in enumerate(portion_order):
        for j in near:
            loading(j, c).wait()
            where = sampled if j else slices
            for i in range(portion_rows // BLOCK_BOXES):
                box = pl.multiple_of(portion_at(c) + i * BLOCK_BOXES, BLOCK_BOXES)
                traces_block = tr[j, pl.ds(pl.multiple_of(box * BOXT, columns), columns), :]
                pair = jnp.dot(mat[...], traces_block, preferred_element_type=jnp.float32)
                pair = pair.astype(jnp.bfloat16)
                for q in range(CHEB):
                    where[j, q, pl.ds(box, BLOCK_BOXES), :] = pair[
                        q * BLOCK_BOXES : (q + 1) * BLOCK_BOXES, :
                    ]
            if j:
                regroup(j, c).start()
        pumps(f"interp{turn}")

    table_copy.wait()
    for turn, c in enumerate(portion_order):
        pumps(f"table{turn}")
        place = pl.ds(portion_at(c), portion_rows)
        total = jnp.zeros((CHEB * portion_rows, 2 * NF), jnp.float32)
        for j in range(n_ta):
            if j:
                regroup(j, c).wait_recv()
            first = pl.multiple_of(flip(ta, j, n_ta) * span, span)
            part = slices[j, :, place, :].reshape(CHEB * portion_rows, span)
            total += jnp.dot(part, fourier[pl.ds(first, span), :], preferred_element_type=jnp.float32)
        mine = pl.ds(portion(c) * per_portion, per_portion)
        for q in range(CHEB):
            points[mine, :, q * 2 * NF : (q + 1) * 2 * NF] = (
                total[q * portion_rows : (q + 1) * portion_rows, :]
                .reshape(per_portion, boxes // groups, 2 * NF)
                .astype(jnp.bfloat16)
            )
        for offset in range((c + 1) * per_portion - 1, c * per_portion - 1, -1):
            if offset:
                moving(offset, True).start()
        pumps(f"spread{turn}")
    arrived[group] = points[group]
    if joined:
        pairs_copy().wait_recv()
        for level in (1, 2):
            select_twin[level - 1] = selection(pairs_twin[pl.ds(level, 1), :])
    pumps("spread")
    for offset in range(1, groups):
        moving(offset, False).wait_recv()

    for k in range(chunks):
        boxes_in = arrived[:, :, k * chunk : (k + 1) * chunk].astype(jnp.float32)
        boxes_in = boxes_in.reshape(boxes, chunk).astype(jnp.bfloat16)
        states[0, k] = jnp.dot(select[0], boxes_in, preferred_element_type=jnp.float32).astype(
            jnp.bfloat16
        )
        exchange(0, k).start()

    per_chunk = chunk // rows

    def weight(level, k, cols):
        piece = weights[level, k * per_chunk : (k + 1) * per_chunk, :, :, cols]
        return piece.reshape(chunk, chunk)

    def dots(left, right):
        return jnp.dot(left, right, preferred_element_type=jnp.float32)

    def columns_of(n):
        return pl.ds(pl.multiple_of(n * chunk, chunk), chunk)

    def first_joined(level):
        pumps(f"own{level}")
        flush(level)
        finish(level, 0, 2 * chunks * per_chunk)

        def piece_of(k, cols):
            return narrow[k, :, :, cols].reshape(chunk, chunk)

        for k in range(chunks):
            turned[k] = dots(select_twin[level - 1], states[level, k]).astype(jnp.bfloat16)

        def own_part(n, carry):
            cols = columns_of(n)
            straight = jnp.zeros((boxes, chunk), jnp.float32)
            for k in range(chunks):
                straight += dots(states[level, k], piece_of(k, cols))
            sums[0, :, cols] = straight
            across = jnp.zeros((boxes, chunk), jnp.float32)
            for k in range(chunks):
                across += dots(turned[k], piece_of(chunks + k, cols))
            sums[1, :, cols] = across
            return carry

        lax.fori_loop(0, chunks // 2, own_part, 0)
        for k in range(chunks):
            pumps(f"level{level}.{k}")
            exchange(level, k).wait_recv()
            aligned = dots(select[level + 1], partner[level, k]).astype(jnp.bfloat16)
            if k < chunks - 1:

                def partner_part(n, carry):
                    cols = columns_of(n)
                    sums[1, :, cols] += dots(partner[level, k], piece_of(k, cols))
                    sums[0, :, cols] += dots(aligned, piece_of(chunks + k, cols))
                    return carry

                lax.fori_loop(0, chunks // 2, partner_part, 0)
            else:
                for r in (1, 0):
                    for n in range(chunks // 2):
                        cols = pl.ds(n * chunk, chunk)
                        if r:
                            last = dots(partner[level, k], piece_of(k, cols))
                        else:
                            last = dots(aligned, piece_of(chunks + k, cols))
                        both_states[r, n] = (sums[r, :, cols] + last).astype(jnp.bfloat16)
                        join(r, n).start()

    def second_joined(level):
        pumps(f"own{level}")
        flush(level)
        finish(level, 0, 2 * chunks * per_chunk)

        def piece_of(n, cols):
            return short[2 * n : 2 * n + 2, :, :, cols].reshape(chunk, chunk)

        for r in (1, 0):

            def own_part(q, carry):
                cols = columns_of(q)
                total = jnp.zeros((boxes, chunk), jnp.float32)
                for n in range(chunks // 2):
                    total += dots(both_states[r, n], piece_of(n, cols))
                sums[r, :, cols] = total
                return carry

            lax.fori_loop(0, chunks, own_part, 0)
        turns = [(r, n) for r in (1, 0) for n in range(chunks // 2)]
        for turn, (r, n) in enumerate(turns):
            if turn < chunks:
                pumps(f"level{level}.{turn}")
            join(r, n).wait_recv()
            table_of = select_twin[level - 1] if r else select[level + 1]
            aligned = dots(table_of, both_partner[r, n]).astype(jnp.bfloat16)
            if n < chunks // 2 - 1:

                def partner_part(q, carry):
                    cols = columns_of(q)
                    sums[r, :, cols] += dots(aligned, piece_of(chunks // 2 + n, cols))
                    return carry

                lax.fori_loop(0, chunks, partner_part, 0)
                continue
            for q in range(chunks):
                cols = pl.ds(q * chunk, chunk)
                total = sums[r, :, cols] + dots(aligned, piece_of(chunks // 2 + n, cols))
                if r:
                    part_out[q] = total.astype(jnp.bfloat16)
                    handing(q).start()
                else:
                    handing(q).wait_recv()
                    total += part_in[q].astype(jnp.float32)
                    states[level + 1, q] = total.astype(jnp.bfloat16)
                    exchange(level + 1, q).start()

    def plain_level(level):
        pumps(f"own{level}")
        flush(level)
        finish(level, 0, chunks * per_chunk)

        def own_part(n, carry):
            cols = pl.ds(pl.multiple_of(n * chunk, chunk), chunk)
            total = jnp.zeros((boxes, chunk), jnp.float32)
            for k in range(chunks):
                total += jnp.dot(
                    states[level, k], weight(level, k, cols), preferred_element_type=jnp.float32
                )
            acc[:, cols] = total
            return carry

        lax.fori_loop(0, chunks, own_part, 0)
        for k in range(chunks):
            pumps(f"level{level}.{k}")
            finish(level, (chunks + k) * per_chunk, per_chunk)
            exchange(level, k).wait_recv()
            aligned = jnp.dot(
                select[level + 1], partner[level, k], preferred_element_type=jnp.float32
            ).astype(jnp.bfloat16)
            if k < chunks - 1:

                def partner_part(n, carry):
                    cols = pl.ds(pl.multiple_of(n * chunk, chunk), chunk)
                    acc[:, cols] += jnp.dot(
                        aligned, weight(level, chunks + k, cols), preferred_element_type=jnp.float32
                    )
                    return carry

                lax.fori_loop(0, chunks, partner_part, 0)
            else:
                for n in range(chunks):
                    cols = pl.ds(n * chunk, chunk)
                    total = acc[:, cols] + jnp.dot(
                        aligned, weight(level, chunks + k, cols), preferred_element_type=jnp.float32
                    )
                    if level < level_count - 1:
                        states[level + 1, n] = total.astype(jnp.bfloat16)
                        exchange(level + 1, n).start()
                    else:
                        out[:, cols] = total.astype(jnp.bfloat16)

    for level in range(level_count):
        if joined and level in (1, 2):
            (first_joined if level == 1 else second_joined)(level)
        else:
            plain_level(level)

    for j in range(1, n_ta):
        for c in range(portions):
            regroup(j, c).wait_send()
    for offset in range(1, groups):
        moving(offset, True).wait_send()
    for level in range(level_count):
        for k in range(chunks):
            if not (joined and level == 2):
                exchange(level, k).wait_send()
    if joined:
        pairs_copy().wait_send()
        for n in range(chunks):
            handing(n).wait_send()
        for r in range(2):
            for n in range(chunks // 2):
                join(r, n).wait_send()
    for outer, condition, make in started:
        guarded(both(outer, condition), lambda: make().wait_send())


def on_device(sizes, traces, interp, translations, leaf_slot, pairing):
    n_gx, n_gy, n_ta = sizes
    groups = n_gx * n_gy
    boxes = leaf_slot.shape[0]
    levels, rows, width = translations.shape
    span = traces.shape[1]
    block = traces.shape[0] // n_ta
    chunk = max(TILE, rows)
    chunks = width // chunk
    table = jnp.asarray(spectrum_table(span * n_ta, NF))
    bf16, f32 = jnp.bfloat16, jnp.float32
    joined = halves_join(sizes, levels, rows, width)

    def extra(shape, kind):
        return pltpu.VMEM(shape if joined else (1,) * (len(shape) - 2) + (16, 128), kind)

    anywhere = pl.BlockSpec(memory_space=pl.ANY)
    vmem = pl.BlockSpec(memory_space=pltpu.VMEM)
    dma = pltpu.SemaphoreType.DMA
    return pl.pallas_call(
        functools.partial(kernel, sizes),
        out_shape=jax.ShapeDtypeStruct((boxes, width), bf16),
        in_specs=[anywhere, vmem, anywhere, vmem, vmem, anywhere],
        out_specs=vmem,
        scratch_shapes=[
            pltpu.VMEM((n_ta, block, span), bf16),
            pltpu.VMEM((levels, groups, 2, rows // 2, width), bf16),
            pltpu.VMEM((CHEB * BLOCK_BOXES, BLOCK_BOXES * BOXT), bf16),
            pltpu.VMEM((n_ta, CHEB, boxes, span), bf16),
            pltpu.VMEM((n_ta, CHEB, boxes, span), bf16),
            pltpu.VMEM(table.shape, bf16),
            pltpu.VMEM((boxes, width), f32),
            pltpu.VMEM((groups, boxes // groups, width), bf16),
            pltpu.VMEM((groups, boxes // groups, width), bf16),
            pltpu.VMEM((levels, chunks, boxes, chunk), bf16),
            pltpu.VMEM((levels, chunks, boxes, chunk), bf16),
            pltpu.VMEM((levels + 1, boxes, boxes), bf16),
            extra((groups, 2, rows // 2, width // 2), bf16),
            extra((groups, 2, rows // 4, width), bf16),
            extra((levels, boxes), jnp.int32),
            extra((2, boxes, boxes), bf16),
            extra((chunks, boxes, chunk), bf16),
            extra((2, chunks // 2, boxes, chunk), bf16),
            extra((2, chunks // 2, boxes, chunk), bf16),
            extra((2, boxes, width), f32),
            extra((chunks, boxes, chunk), bf16),
            extra((chunks, boxes, chunk), bf16),
            dma((n_ta, min(4, groups))),
            dma,
            dma((levels, 2, chunks)),
            dma((1,)),
            dma((levels, groups)),
            dma((levels, 2, groups)),
            dma((levels, max(1, n_gx.bit_length() - 1), groups)),
            dma((levels, groups)),
            dma((levels, groups)),
            dma((levels, 2, groups)),
            dma((levels, 2, groups)),
            dma((n_ta, min(4, groups))),
            dma((n_ta, min(4, groups))),
            dma((groups,)),
            dma((groups,)),
            dma((levels, chunks)),
            dma((levels, chunks)),
            dma((2,)),
            dma((2, max(1, chunks // 2))),
            dma((2, max(1, chunks // 2))),
            dma((chunks,)),
            dma((chunks,)),
        ],
        compiler_params=pltpu.CompilerParams(
            collective_id=0, has_side_effects=True, vmem_limit_bytes=60 * 2**20
        ),
    )(traces, interp, translations, leaf_slot.reshape(1, boxes), pairing, table)


def solution(mesh):
    sizes = (mesh.shape["gx"], mesh.shape["gy"], mesh.shape["ta"])
    in_specs = (
        P(("gx", "gy"), "ta"),
        P(),
        P(None, ("gx", "gy"), None),
        P(("gx", "gy", "ta")),
        P(None, ("gx", "gy", "ta")),
    )
    out_specs = P(("gx", "gy", "ta"), None)
    return jax.shard_map(
        functools.partial(on_device, sizes),
        mesh=mesh,
        in_specs=in_specs,
        out_specs=out_specs,
        check_vma=False,
    )
```

```python
import functools
import math

import jax
import jax.numpy as jnp
import numpy as np
from jax import lax
from jax.experimental import pallas as pl
from jax.experimental.pallas import tpu as pltpu
from jax.sharding import PartitionSpec as P

NF = 256
CHEB = 2
BOXT = 16
BLOCK_BOXES = 16
TILE = 256
MESH = pl.DeviceIdType.MESH
KEPT = (0.625, 0.5, 0.875, 1)
SCHEDULE = {
    "start": ((0, 0, 0, -1), (1, 2, 0, 1), (1, 3, 0, 1),),
    "interp0": ((0, 2, 0, -1), (1, 1, 1, -1),),
    "interp1": ((0, 0, 0, 0),),
    "interp3": ((1, 1, 0, 1),),
    "spread0": ((1, 1, 1, 1), (1, 2, 1, 2), (1, 0, 0, 0), (0, 0, 0, 2), (0, 0, 1, 0),),
    "table1": ((0, 0, 1, -1), (1, 1, 0, 2), (0, 0, 0, 1), (0, 1, 0, -1),),
    "spread2": (
        (1, 0, 1, 0),
        (0, 2, 1, -1),
        (1, 0, 0, 2),
        (1, 1, 1, 0),
        (0, 0, 1, 1),
        (1, 2, 1, -1),
        (0, 1, 0, 0),
        (0, 0, 1, 2),
    ),
    "table3": ((1, 0, 0, 1), (1, 3, 1, -1),),
    "spread3": (
        (1, 3, 1, 1),
        (0, 1, 0, 1),
        (1, 3, 0, 0),
        (1, 0, 1, 2),
        (1, 3, 0, 2),
        (0, 3, 0, -1),
        (0, 1, 1, -1),
    ),
    "spread": ((1, 0, 1, 1), (1, 0, 1, -1),),
    "level0.0": ((0, 1, 0, 2),),
    "level0.3": ((0, 2, 0, 0),),
    "own1": (
        (0, 1, 1, 0),
        (0, 1, 1, 2),
        (1, 1, 0, 0),
        (0, 1, 1, 1),
        (0, 2, 0, 1),
        (1, 1, 1, 2),
        (0, 2, 0, 2),
    ),
    "level1.1": ((0, 3, 0, 0), (1, 2, 1, 1),),
    "level1.2": ((1, 2, 0, 2),),
    "level1.3": ((1, 3, 1, 2), (1, 2, 1, 0), (1, 2, 0, 0),),
    "own2": ((0, 2, 1, 1), (0, 2, 1, 0), (0, 2, 1, 2),),
    "level2.0": ((0, 3, 0, 1),),
    "level2.2": ((1, 3, 1, 0),),
    "level2.3": ((0, 3, 1, 0), (0, 3, 1, -1),),
    "own3": ((0, 3, 1, 1), (0, 3, 0, 2), (0, 3, 1, 2),),
}


def spectrum_table(length, count):
    sample_pos = np.arange(length, dtype=np.float32)[:, None]
    frequency = np.arange(count, dtype=np.float32)[None, :] + np.float32(1.0)
    angles = np.float32(2.0 * math.pi / length) * np.mod(sample_pos * frequency, np.float32(length))
    factor = np.float32(math.sqrt(2.0 / length))
    table = np.concatenate([np.cos(angles) * factor, -np.sin(angles) * factor], axis=1)
    return table.astype(jnp.bfloat16)


def flip(index, mask, size):
    result = index
    bit = 1
    while bit < size:
        if mask & bit:
            result = result + bit - 2 * bit * ((index // bit) % 2)
        bit *= 2
    return result


def mask_of(level, levels, devices):
    return 2 ** (level * (devices.bit_length() - 1) // levels)


def halves_join(sizes, levels, rows, width):
    n_gx, n_gy, n_ta = sizes
    devices = n_gx * n_gy * n_ta
    return (
        levels == 4
        and n_ta >= 4
        and mask_of(1, levels, devices) == 2
        and mask_of(2, levels, devices) >= n_ta
        and rows >= TILE
        and rows == max(TILE, rows)
        and width // rows >= 2
        and rows * n_gx * n_gy == 2 * width
    )


def kernel(
    sizes,
    traces,
    interp,
    translations,
    slots,
    pairs,
    table,
    out,
    tr,
    weights,
    mat,
    sampled,
    slices,
    fourier,
    acc,
    points,
    arrived,
    states,
    partner,
    select,
    narrow,
    short,
    pairs_twin,
    select_twin,
    turned,
    both_states,
    both_partner,
    sums,
    part_out,
    part_in,
    load_sem,
    table_sem,
    own_sem,
    ag_send,
    ag_recv,
    z_send,
    x_send,
    y_send,
    y_recv,
    core_send,
    core_recv,
    ta_send,
    ta_recv,
    g_send,
    g_recv,
    level_send,
    level_recv,
    pairs_sem,
    join_send,
    join_recv,
    part_send,
    part_recv,
):
    n_gx, n_gy, n_ta = sizes
    groups = n_gx * n_gy
    gx, gy, ta = lax.axis_index("gx"), lax.axis_index("gy"), lax.axis_index("ta")
    group = gx * n_gy + gy
    level_count = translations.shape[0]
    rows = translations.shape[1]
    half = rows // 2
    width = translations.shape[2]
    boxes = slots.shape[1]
    span = traces.shape[1]
    block = boxes * BOXT
    chunk = states.shape[3]
    chunks = width // chunk
    log_devices = (groups * n_ta).bit_length() - 1
    side = ta % 2

    def of_group(offset):
        p = flip(group, offset, groups)
        return (p // n_gy, p % n_gy, ta)

    def of_ta(offset):
        return (gx, gy, flip(ta, offset, n_ta))

    upper = (ta // 2) % 2
    joined = halves_join(sizes, level_count, rows, width)

    def own(level):
        if joined and level == 1:
            strip = chunk // 2
            return [
                pltpu.make_async_copy(
                    translations.at[
                        level,
                        pl.ds(part * half, half),
                        pl.ds(pl.multiple_of(k * chunk + upper * strip, strip), strip),
                    ],
                    narrow.at[group, part, :, pl.ds(k * strip, strip)],
                    own_sem.at[level, part, k],
                )
                for part in range(2)
                for k in range(chunks)
            ]
        if joined and level == 2:
            quarter = half // 2
            return [
                pltpu.make_async_copy(
                    translations.at[
                        level,
                        pl.ds(pl.multiple_of(upper * half + part * quarter, quarter), quarter),
                        :,
                    ],
                    short.at[group, part],
                    own_sem.at[level, part, 0],
                )
                for part in range(2)
            ]
        return [
            pltpu.make_async_copy(
                translations.at[level, pl.ds(part * half, half), :],
                weights.at[level, group, part],
                own_sem.at[level, part, 0],
            )
            for part in range(2)
        ]

    xbits = []
    bit = n_gx // 2
    while bit:
        xbits.append(bit)
        bit //= 2
    stage_of = {0: -1}
    for stage, bit in enumerate(xbits):
        for offset in list(stage_of):
            stage_of[offset ^ bit] = stage
    lines = {offset: flip(gx, offset, n_gx) for offset in stage_of}
    shards = [
        (offset, d, k)
        for k in range(-1, n_gy - 1)
        for d in ((1,) if k < 0 else (1, -1))
        for offset in stage_of
    ]
    twins = n_ta >= 4
    twin = flip(ta, 2, n_ta) if twins else ta

    def kept(level):
        if not twins or (joined and level in (1, 2)):
            return half
        return max(half // 2, round(half * KEPT[level % len(KEPT)] / 16) * 16)

    def shard_id(offset, d, k):
        return lines[offset] * n_gy + gy - d * (k + 1)

    within = {
        (d, k): gy >= k + 1 if d > 0 else gy < n_gy - 1 - k
        for d in (1, -1)
        for k in range(n_gy - 1)
    }
    ahead = {1: gy < n_gy - 1, -1: gy > 0}

    def inside(d, k):
        return None if k < 0 else within[d, k]

    def both(a, b):
        if a is None or b is None:
            return b if a is None else a
        return jnp.logical_and(a, b)

    def guarded(condition, action):
        if condition is None:
            action()
        else:
            pl.when(condition)(action)

    started = []

    def launch(condition, make, outer=None):
        guarded(condition, lambda: make().start())
        started.append((outer, condition, make))

    def in_rows(level):
        size = kept(level)
        if size == half:
            return pl.ds(0, half)
        return pl.ds(pl.multiple_of(upper * (half - size), 16), size)

    def held(level, shard, part):
        if joined and level == 1:
            return narrow.at[shard, part]
        if joined and level == 2:
            return short.at[shard, part]
        return weights.at[level, shard, part, in_rows(level), :]

    def in_plane(level, shard, sem_ref, sem_at, target):
        place = held(level, shard, side)
        return pltpu.make_async_remote_copy(
            src_ref=place,
            dst_ref=place,
            send_sem=sem_ref.at[sem_at],
            recv_sem=ag_recv.at[level, shard],
            device_id=target,
            device_id_type=MESH,
        )

    def z_copy(level, shard, d):
        return in_plane(level, shard, z_send, (level, (d + 1) // 2, shard), (gx, gy + d, ta))

    def x_copy(level, shard, stage):
        target = (lines[xbits[stage]], gy, ta)
        return in_plane(level, shard, x_send, (level, stage, shard), target)

    def y_copy(level, shard, sending):
        size = kept(level)
        first = (upper if sending else 1 - upper) * size
        place = weights.at[level, shard, side, pl.ds(pl.multiple_of(first, 16), half - size), :]
        return pltpu.make_async_remote_copy(
            src_ref=place,
            dst_ref=place,
            send_sem=y_send.at[level, shard],
            recv_sem=y_recv.at[level, shard],
            device_id=(gx, gy, twin),
            device_id_type=MESH,
        )

    def core_copy(level, shard, kind, mine):
        size = kept(level)
        part = side if mine else 1 - side
        if kind == 0:
            place = held(level, shard, part)
        else:
            rows_at = pl.ds(pl.multiple_of((1 - upper) * size, 16), half - size)
            place = weights.at[level, shard, part, rows_at, :]
        return pltpu.make_async_remote_copy(
            src_ref=place,
            dst_ref=place,
            send_sem=core_send.at[level, kind, shard],
            recv_sem=core_recv.at[level, kind, shard],
            device_id=of_ta(1),
            device_id_type=MESH,
        )

    def has_twin(level):
        return kept(level) < half

    def forward(level, offset, d, k):
        shard = shard_id(offset, d, k)
        valid = inside(d, k)
        own_shard = offset == 0 and k < 0

        def body():
            if not own_shard:
                in_plane(level, shard, ag_send, 0, of_ta(1)).wait_recv()
                launch(None, lambda: core_copy(level, shard, 0, True), valid)
            if offset == 0:
                for way in (1, -1) if k < 0 else (d,):
                    launch(ahead[way], lambda way=way: z_copy(level, shard, way), valid)
            for stage in range(stage_of[offset] + 1, len(xbits)):
                launch(None, lambda stage=stage: x_copy(level, shard, stage), valid)
            if has_twin(level) and not own_shard:
                launch(None, lambda: y_copy(level, shard, True), valid)

        guarded(valid, body)

    def crossed(level, offset, d, k):
        shard = shard_id(offset, d, k)

        def body():
            y_copy(level, shard, False).wait_recv()
            launch(None, lambda: core_copy(level, shard, 1, True), inside(d, k))

        guarded(inside(d, k), body)

    handled = set()

    def piece(across, level, over, k):
        if (across, level, over, k) in handled or level >= level_count or k > n_gy - 2:
            return
        handled.add((across, level, over, k))
        if not (across or over) and k >= 0:
            piece(0, level, 0, k - 1)
        if across and not has_twin(level):
            return
        if k < 0 and not (across or over):
            for copy in own(level):
                copy.wait()
        for offset, d, at in shards:
            if at == k and (offset > 0) == (over > 0):
                if not across:
                    forward(level, offset, d, k)
                elif offset or k >= 0:
                    crossed(level, offset, d, k)

    def pumps(point):
        for entry in SCHEDULE.get(point, ()):
            piece(*entry)

    def flush(level):
        for across in range(2):
            for total in range(-1, n_gy):
                for over in range(2):
                    if -1 <= total - over < n_gy - 1:
                        piece(across, level, over, total - over)

    def finish(level, first, count):
        for shard in range(first, first + count):

            def body():
                core_copy(level, shard, 0, False).wait_recv()
                if has_twin(level):
                    core_copy(level, shard, 1, False).wait_recv()

            pl.when(group != shard)(body)

    portions = min(4, groups)
    per_portion = groups // portions
    portion_rows = boxes // portions
    portion_order = sorted(range(portions), key=lambda c: (-(c % 2), -c))

    def portion(c):
        return flip(group // per_portion, c, portions)

    def portion_at(c):
        return pl.multiple_of(portion(c) * portion_rows, portion_rows)

    def loading(j, c):
        size = portion_rows * BOXT
        first = pl.multiple_of(portion(c) * size, size)
        source = pl.multiple_of(flip(ta, j, n_ta) * block + first, size)
        return pltpu.make_async_copy(
            traces.at[pl.ds(source, size), :], tr.at[j, pl.ds(first, size), :], load_sem.at[j, c]
        )

    def regroup(j, c):
        place = pl.ds(portion_at(c), portion_rows)
        return pltpu.make_async_remote_copy(
            src_ref=sampled.at[j, :, place, :],
            dst_ref=slices.at[j, :, place, :],
            send_sem=ta_send.at[j, c],
            recv_sem=ta_recv.at[j, c],
            device_id=of_ta(j),
            device_id_type=MESH,
        )

    def moving(offset, sending):
        src = points.at[flip(group, offset, groups)]
        dst = arrived.at[group if sending else flip(group, offset, groups)]
        return pltpu.make_async_remote_copy(
            src_ref=src,
            dst_ref=dst,
            send_sem=g_send.at[offset],
            recv_sem=g_recv.at[offset],
            device_id=of_group(offset),
            device_id_type=MESH,
        )

    def exchange(level, k):
        mask = 2 ** (level * log_devices // level_count)
        target = of_ta(mask) if mask < n_ta else of_group(mask // n_ta)
        return pltpu.make_async_remote_copy(
            src_ref=states.at[level, k],
            dst_ref=partner.at[level, k],
            send_sem=level_send.at[level, k],
            recv_sem=level_recv.at[level, k],
            device_id=target,
            device_id_type=MESH,
        )

    def twin_copy(src, dst, sems):
        return pltpu.make_async_remote_copy(
            src_ref=src,
            dst_ref=dst,
            send_sem=sems[0],
            recv_sem=sems[1],
            device_id=of_ta(2),
            device_id_type=MESH,
        )

    def pairs_copy():
        return twin_copy(pairs, pairs_twin, (pairs_sem.at[0], pairs_sem.at[1]))

    def handing(n):
        return twin_copy(part_out.at[n], part_in.at[n], (part_send.at[n], part_recv.at[n]))

    def join(r, n):
        return pltpu.make_async_remote_copy(
            src_ref=both_states.at[r, n],
            dst_ref=both_partner.at[r, n],
            send_sem=join_send.at[r, n],
            recv_sem=join_recv.at[r, n],
            device_id=of_group(mask_of(2, level_count, groups * n_ta) // n_ta),
            device_id_type=MESH,
        )

    near = [n_ta - 1 - j for j in range(n_ta)]
    table_copy = pltpu.make_async_copy(table, fourier, table_sem)
    for copy in own(0):
        copy.start()
    for turn, c in enumerate(portion_order):
        for j in near:
            loading(j, c).start()
        if turn == 0:
            table_copy.start()
            for copy in own(1):
                copy.start()
    for level in range(2, level_count):
        for copy in own(level):
            copy.start()

    barrier = pltpu.get_barrier_semaphore()
    for j in range(1, n_ta):
        pl.semaphore_signal(barrier, inc=1, device_id=of_ta(j), device_id_type=MESH)
    for offset in range(1, groups):
        pl.semaphore_signal(barrier, inc=1, device_id=of_group(offset), device_id_type=MESH)

    columns = BLOCK_BOXES * BOXT
    spread = (
        lax.broadcasted_iota(jnp.int32, (BOXT, columns), 1) % BOXT
        == lax.broadcasted_iota(jnp.int32, (BOXT, columns), 0)
    )
    tiled = jnp.dot(
        interp[...], spread.astype(jnp.float32).astype(jnp.bfloat16), preferred_element_type=jnp.float32
    )
    own_box = (
        lax.broadcasted_iota(jnp.int32, (BLOCK_BOXES, columns), 1) // BOXT
        == lax.broadcasted_iota(jnp.int32, (BLOCK_BOXES, columns), 0)
    )
    for c in range(CHEB):
        mat[pl.ds(c * BLOCK_BOXES, BLOCK_BOXES), :] = jnp.where(
            own_box, tiled[c : c + 1, :], 0.0
        ).astype(jnp.bfloat16)

    def selection(index_row):
        hit = lax.broadcasted_iota(jnp.int32, (boxes, boxes), 0) == index_row
        return jnp.where(hit, 1.0, 0.0).T.astype(jnp.bfloat16)

    select[0] = selection(slots[...])
    for level in range(level_count):
        select[level + 1] = selection(pairs[pl.ds(level, 1), :])

    pl.semaphore_wait(barrier, n_ta - 1 + groups - 1)
    pumps("start")
    if joined:
        pairs_copy().start()

    for turn, c in enumerate(portion_order):
        for j in near:
            loading(j, c).wait()
            where = sampled if j else slices
            for i in range(portion_rows // BLOCK_BOXES):
                box = pl.multiple_of(portion_at(c) + i * BLOCK_BOXES, BLOCK_BOXES)
                traces_block = tr[j, pl.ds(pl.multiple_of(box * BOXT, columns), columns), :]
                pair = jnp.dot(mat[...], traces_block, preferred_element_type=jnp.float32)
                pair = pair.astype(jnp.bfloat16)
                for q in range(CHEB):
                    where[j, q, pl.ds(box, BLOCK_BOXES), :] = pair[
                        q * BLOCK_BOXES : (q + 1) * BLOCK_BOXES, :
                    ]
            if j:
                regroup(j, c).start()
        pumps(f"interp{turn}")

    table_copy.wait()
    for turn, c in enumerate(portion_order):
        pumps(f"table{turn}")
        place = pl.ds(portion_at(c), portion_rows)
        total = jnp.zeros((CHEB * portion_rows, 2 * NF), jnp.float32)
        for j in range(n_ta):
            if j:
                regroup(j, c).wait_recv()
            first = pl.multiple_of(flip(ta, j, n_ta) * span, span)
            part = slices[j, :, place, :].reshape(CHEB * portion_rows, span)
            total += jnp.dot(part, fourier[pl.ds(first, span), :], preferred_element_type=jnp.float32)
        mine = pl.ds(portion(c) * per_portion, per_portion)
        for q in range(CHEB):
            points[mine, :, q * 2 * NF : (q + 1) * 2 * NF] = (
                total[q * portion_rows : (q + 1) * portion_rows, :]
                .reshape(per_portion, boxes // groups, 2 * NF)
                .astype(jnp.bfloat16)
            )
        for offset in range((c + 1) * per_portion - 1, c * per_portion - 1, -1):
            if offset:
                moving(offset, True).start()
        pumps(f"spread{turn}")
    arrived[group] = points[group]
    if joined:
        pairs_copy().wait_recv()
        for level in (1, 2):
            select_twin[level - 1] = selection(pairs_twin[pl.ds(level, 1), :])
    pumps("spread")
    for offset in range(1, groups):
        moving(offset, False).wait_recv()

    for k in range(chunks):
        boxes_in = arrived[:, :, k * chunk : (k + 1) * chunk].astype(jnp.float32)
        boxes_in = boxes_in.reshape(boxes, chunk).astype(jnp.bfloat16)
        states[0, k] = jnp.dot(select[0], boxes_in, preferred_element_type=jnp.float32).astype(
            jnp.bfloat16
        )
        exchange(0, k).start()

    per_chunk = chunk // rows

    def weight(level, k, cols):
        piece = weights[level, k * per_chunk : (k + 1) * per_chunk, :, :, cols]
        return piece.reshape(chunk, chunk)

    def dots(left, right):
        return jnp.dot(left, right, preferred_element_type=jnp.float32)

    def columns_of(n):
        return pl.ds(pl.multiple_of(n * chunk, chunk), chunk)

    def first_joined(level):
        pumps(f"own{level}")
        flush(level)
        finish(level, 0, 2 * chunks * per_chunk)

        def piece_of(k, cols):
            return narrow[k, :, :, cols].reshape(chunk, chunk)

        for k in range(chunks):
            turned[k] = dots(select_twin[level - 1], states[level, k]).astype(jnp.bfloat16)

        def own_part(n, carry):
            cols = columns_of(n)
            straight = jnp.zeros((boxes, chunk), jnp.float32)
            for k in range(chunks):
                straight += dots(states[level, k], piece_of(k, cols))
            sums[0, :, cols] = straight
            across = jnp.zeros((boxes, chunk), jnp.float32)
            for k in range(chunks):
                across += dots(turned[k], piece_of(chunks + k, cols))
            sums[1, :, cols] = across
            return carry

        lax.fori_loop(0, chunks // 2, own_part, 0)
        for k in range(chunks):
            pumps(f"level{level}.{k}")
            exchange(level, k).wait_recv()
            aligned = dots(select[level + 1], partner[level, k]).astype(jnp.bfloat16)
            if k < chunks - 1:

                def partner_part(n, carry):
                    cols = columns_of(n)
                    sums[1, :, cols] += dots(partner[level, k], piece_of(k, cols))
                    sums[0, :, cols] += dots(aligned, piece_of(chunks + k, cols))
                    return carry

                lax.fori_loop(0, chunks // 2, partner_part, 0)
            else:
                for r in (1, 0):
                    for n in range(chunks // 2):
                        cols = pl.ds(n * chunk, chunk)
                        if r:
                            last = dots(partner[level, k], piece_of(k, cols))
                        else:
                            last = dots(aligned, piece_of(chunks + k, cols))
                        both_states[r, n] = (sums[r, :, cols] + last).astype(jnp.bfloat16)
                        join(r, n).start()

    def second_joined(level):
        pumps(f"own{level}")
        flush(level)
        finish(level, 0, 2 * chunks * per_chunk)

        def piece_of(n, cols):
            return short[2 * n : 2 * n + 2, :, :, cols].reshape(chunk, chunk)

        for r in (1, 0):

            def own_part(q, carry):
                cols = columns_of(q)
                total = jnp.zeros((boxes, chunk), jnp.float32)
                for n in range(chunks // 2):
                    total += dots(both_states[r, n], piece_of(n, cols))
                sums[r, :, cols] = total
                return carry

            lax.fori_loop(0, chunks, own_part, 0)
        turns = [(r, n) for r in (1, 0) for n in range(chunks // 2)]
        for turn, (r, n) in enumerate(turns):
            if turn < chunks:
                pumps(f"level{level}.{turn}")
            join(r, n).wait_recv()
            table_of = select_twin[level - 1] if r else select[level + 1]
            aligned = dots(table_of, both_partner[r, n]).astype(jnp.bfloat16)
            if n < chunks // 2 - 1:

                def partner_part(q, carry):
                    cols = columns_of(q)
                    sums[r, :, cols] += dots(aligned, piece_of(chunks // 2 + n, cols))
                    return carry

                lax.fori_loop(0, chunks, partner_part, 0)
                continue
            for q in range(chunks):
                cols = pl.ds(q * chunk, chunk)
                total = sums[r, :, cols] + dots(aligned, piece_of(chunks // 2 + n, cols))
                if r:
                    part_out[q] = total.astype(jnp.bfloat16)
                    handing(q).start()
                else:
                    handing(q).wait_recv()
                    total += part_in[q].astype(jnp.float32)
                    states[level + 1, q] = total.astype(jnp.bfloat16)
                    exchange(level + 1, q).start()

    def plain_level(level):
        pumps(f"own{level}")
        flush(level)
        finish(level, 0, chunks * per_chunk)

        def own_part(n, carry):
            cols = pl.ds(pl.multiple_of(n * chunk, chunk), chunk)
            total = jnp.zeros((boxes, chunk), jnp.float32)
            for k in range(chunks):
                total += jnp.dot(
                    states[level, k], weight(level, k, cols), preferred_element_type=jnp.float32
                )
            acc[:, cols] = total
            return carry

        lax.fori_loop(0, chunks, own_part, 0)
        for k in range(chunks):
            pumps(f"level{level}.{k}")
            finish(level, (chunks + k) * per_chunk, per_chunk)
            exchange(level, k).wait_recv()
            aligned = jnp.dot(
                select[level + 1], partner[level, k], preferred_element_type=jnp.float32
            ).astype(jnp.bfloat16)
            if k < chunks - 1:

                def partner_part(n, carry):
                    cols = pl.ds(pl.multiple_of(n * chunk, chunk), chunk)
                    acc[:, cols] += jnp.dot(
                        aligned, weight(level, chunks + k, cols), preferred_element_type=jnp.float32
                    )
                    return carry

                lax.fori_loop(0, chunks, partner_part, 0)
            else:
                for n in range(chunks):
                    cols = pl.ds(n * chunk, chunk)
                    total = acc[:, cols] + jnp.dot(
                        aligned, weight(level, chunks + k, cols), preferred_element_type=jnp.float32
                    )
                    if level < level_count - 1:
                        states[level + 1, n] = total.astype(jnp.bfloat16)
                        exchange(level + 1, n).start()
                    else:
                        out[:, cols] = total.astype(jnp.bfloat16)

    for level in range(level_count):
        if joined and level in (1, 2):
            (first_joined if level == 1 else second_joined)(level)
        else:
            plain_level(level)

    for j in range(1, n_ta):
        for c in range(portions):
            regroup(j, c).wait_send()
    for offset in range(1, groups):
        moving(offset, True).wait_send()
    for level in range(level_count):
        for k in range(chunks):
            if not (joined and level == 2):
                exchange(level, k).wait_send()
    if joined:
        pairs_copy().wait_send()
        for n in range(chunks):
            handing(n).wait_send()
        for r in range(2):
            for n in range(chunks // 2):
                join(r, n).wait_send()
    for outer, condition, make in started:
        guarded(both(outer, condition), lambda: make().wait_send())


def on_device(sizes, traces, interp, translations, leaf_slot, pairing):
    n_gx, n_gy, n_ta = sizes
    groups = n_gx * n_gy
    boxes = leaf_slot.shape[0]
    levels, rows, width = translations.shape
    span = traces.shape[1]
    block = traces.shape[0] // n_ta
    chunk = max(TILE, rows)
    chunks = width // chunk
    table = jnp.asarray(spectrum_table(span * n_ta, NF))
    bf16, f32 = jnp.bfloat16, jnp.float32
    joined = halves_join(sizes, levels, rows, width)

    def extra(shape, kind):
        return pltpu.VMEM(shape if joined else (1,) * (len(shape) - 2) + (16, 128), kind)

    anywhere = pl.BlockSpec(memory_space=pl.ANY)
    vmem = pl.BlockSpec(memory_space=pltpu.VMEM)
    dma = pltpu.SemaphoreType.DMA
    return pl.pallas_call(
        functools.partial(kernel, sizes),
        out_shape=jax.ShapeDtypeStruct((boxes, width), bf16),
        in_specs=[anywhere, vmem, anywhere, vmem, vmem, anywhere],
        out_specs=vmem,
        scratch_shapes=[
            pltpu.VMEM((n_ta, block, span), bf16),
            pltpu.VMEM((levels, groups, 2, rows // 2, width), bf16),
            pltpu.VMEM((CHEB * BLOCK_BOXES, BLOCK_BOXES * BOXT), bf16),
            pltpu.VMEM((n_ta, CHEB, boxes, span), bf16),
            pltpu.VMEM((n_ta, CHEB, boxes, span), bf16),
            pltpu.VMEM(table.shape, bf16),
            pltpu.VMEM((boxes, width), f32),
            pltpu.VMEM((groups, boxes // groups, width), bf16),
            pltpu.VMEM((groups, boxes // groups, width), bf16),
            pltpu.VMEM((levels, chunks, boxes, chunk), bf16),
            pltpu.VMEM((levels, chunks, boxes, chunk), bf16),
            pltpu.VMEM((levels + 1, boxes, boxes), bf16),
            extra((groups, 2, rows // 2, width // 2), bf16),
            extra((groups, 2, rows // 4, width), bf16),
            extra((levels, boxes), jnp.int32),
            extra((2, boxes, boxes), bf16),
            extra((chunks, boxes, chunk), bf16),
            extra((2, chunks // 2, boxes, chunk), bf16),
            extra((2, chunks // 2, boxes, chunk), bf16),
            extra((2, boxes, width), f32),
            extra((chunks, boxes, chunk), bf16),
            extra((chunks, boxes, chunk), bf16),
            dma((n_ta, min(4, groups))),
            dma,
            dma((levels, 2, chunks)),
            dma((1,)),
            dma((levels, groups)),
            dma((levels, 2, groups)),
            dma((levels, max(1, n_gx.bit_length() - 1), groups)),
            dma((levels, groups)),
            dma((levels, groups)),
            dma((levels, 2, groups)),
            dma((levels, 2, groups)),
            dma((n_ta, min(4, groups))),
            dma((n_ta, min(4, groups))),
            dma((groups,)),
            dma((groups,)),
            dma((levels, chunks)),
            dma((levels, chunks)),
            dma((2,)),
            dma((2, max(1, chunks // 2))),
            dma((2, max(1, chunks // 2))),
            dma((chunks,)),
            dma((chunks,)),
        ],
        compiler_params=pltpu.CompilerParams(
            collective_id=0, has_side_effects=True, vmem_limit_bytes=60 * 2**20
        ),
    )(traces, interp, translations, leaf_slot.reshape(1, boxes), pairing, table)


def solution(mesh):
    sizes = (mesh.shape["gx"], mesh.shape["gy"], mesh.shape["ta"])
    in_specs = (
        P(("gx", "gy"), "ta"),
        P(),
        P(None, ("gx", "gy"), None),
        P(("gx", "gy", "ta")),
        P(None, ("gx", "gy", "ta")),
    )
    out_specs = P(("gx", "gy", "ta"), None)
    return jax.shard_map(
        functools.partial(on_device, sizes),
        mesh=mesh,
        in_specs=in_specs,
        out_specs=out_specs,
        check_vma=False,
    )
```
